32 devices in a mesh: tm: 4 (over z), rows: 8 (over y, x, core).
Axes of the slice: x: 2, y: 2, z: 4, core: 2. Of those that a mesh axis runs over, the one named last changes fastest.
Arguments:
- feat_mid: bfloat16 [16, 64, 128, 256], P('tm', 'rows'), may hold values from -15 to 15
- gain_mid: float32 [256], replicated, may hold values from 0.1 to 1.9
- conv_mid: bfloat16 [3, 3, 3, 256, 256], replicated, may hold values from -0.078125 to 0.078125
- down_weight: bfloat16 [8, 256, 512], replicated, may hold values from -0.125 to 0.125
- wavelets: bfloat16 [8, 24, 32, 64], P('tm', None, 'rows'), may hold values from -6 to 6
- inject_weight: bfloat16 [24, 512], replicated, may hold values from -1.25 to 1.25
- gain_deep: float32 [512], replicated, may hold values from 0.1 to 1.9
- conv_deep: bfloat16 [3, 3, 3, 512, 512], replicated, may hold values from -0.0546875 to 0.0546875
Outputs:
- encoded: bfloat16 [8, 32, 64, 512], P('tm', 'rows')
The draws below stay inside these ranges and needn't reach their ends.
All inputs are finite; a program needn't handle non-finite values.
Results may differ from the reference program's by a relative error of at most 0.0095.
Values may be sent and summed in bfloat16 or wider, within the bound.
No kernel may reach another device: no remote copies, remote signals or barrier semaphores. Data moves between devices by JAX's collectives and lax.ppermute only.
A program may use at most 256 MiB of HBM per device.

```python
import math
import jax
import jax.numpy as jnp
from jax import lax

CH_MID = 256
CH_DEEP = 512
COLUMNS = 128
BANDS = 24
FRAMES = 16
IMG_ROWS = 64


def draw_feat_mid(key, part):
    channel_key = jax.random.fold_in(key, 11)
    value_key = jax.random.fold_in(key, 23)
    scales = jnp.exp(jax.random.uniform(channel_key, (CH_MID,), jnp.float32, math.log(0.3), math.log(3.0)))
    shape = (FRAMES, IMG_ROWS, COLUMNS, CH_MID)
    values = jnp.clip(jax.random.normal(value_key, shape, jnp.float32), -5.0, 5.0) * scales
    return values.astype(jnp.bfloat16)


def block_levels(rng, dims, pieces, least, top_value):
    level, own = 1.0, jax.random.fold_in(rng, 6)
    for dim, parts in pieces:
        draws = jnp.exp(jax.random.uniform(jax.random.fold_in(own, dim), (parts,), jnp.float32, least / len(pieces), top_value / len(pieces)))
        level = level * jnp.repeat(draws, dims[dim] // parts).reshape([-1 if axis == dim else 1 for axis in range(len(dims))])
    return level


def bell_draw(own_key, dims, width, limit, cuts=(), kind=jnp.bfloat16):
    values = jax.random.normal(own_key, dims, jnp.float32) * width
    if len(cuts) > 0:
        values = block_levels(own_key, dims, cuts, -0.22, 0.18) * values
    return jnp.clip(values, min=-limit, max=limit).astype(kind)


def setup_inputs(seed: int = 0) -> dict:
    arg_keys = jax.random.split(jax.random.key(seed), 9)
    feat_mid = draw_feat_mid(jax.random.fold_in(arg_keys[8], 71), 0)
    gain_mid = jnp.clip(1.0 + 0.18 * jax.random.normal(arg_keys[1], (CH_MID,), jnp.float32), 0.1, 1.9)
    conv_mid = bell_draw(arg_keys[2], (3, 3, 3, CH_MID, CH_MID), (27 * CH_MID) ** -0.5, 0.078125)
    down_weight = bell_draw(arg_keys[3], (8, CH_MID, CH_DEEP), (8 * CH_MID) ** -0.5, 0.125)
    wavelets = bell_draw(arg_keys[4], (FRAMES // 2, BANDS, IMG_ROWS // 2, COLUMNS // 2), 1.0, 6.0, ((0, 4), (2, 8)))
    inject_weight = bell_draw(arg_keys[5], (BANDS, CH_DEEP), BANDS ** -0.5, 1.25)
    gain_deep = jnp.clip(1.0 + 0.18 * jax.random.normal(arg_keys[6], (CH_DEEP,), jnp.float32), 0.1, 1.9)
    conv_deep = bell_draw(arg_keys[7], (3, 3, 3, CH_DEEP, CH_DEEP), (27 * CH_DEEP) ** -0.5, 0.0546875)
    return {"feat_mid": feat_mid, "gain_mid": gain_mid, "conv_mid": conv_mid, "down_weight": down_weight, "wavelets": wavelets, "inject_weight": inject_weight, "gain_deep": gain_deep, "conv_deep": conv_deep}


epsilon = 1e-06
haar_scale = 0.35355339059327373

def norm_act(values, scales):
    average = lax.optimization_barrier(jnp.mean(values, axis=-1, keepdims=True))
    centred = values - average
    spread = lax.optimization_barrier(jnp.mean(centred * centred, axis=-1, keepdims=True))
    return jax.nn.silu(centred * lax.rsqrt(spread + epsilon) * scales).astype(jnp.bfloat16)

def causal_conv(normed, weight):
    frames, height, breadth, channels = normed.shape
    padded = jnp.pad(normed, ((2, 0), (1, 1), (1, 1), (0, 0)))

    def one_frame(frame_index):
        window = lax.dynamic_slice_in_dim(padded, frame_index, 3, 0)
        summed = jnp.zeros((height * breadth, weight.shape[-1]), jnp.float32)
        for depth_tap in range(3):
            for row_tap in range(3):
                for col_tap in range(3):
                    flattened = window[depth_tap, row_tap:row_tap + height, col_tap:col_tap + breadth].reshape(height * breadth, channels)
                    summed = summed + jnp.dot(flattened, weight[depth_tap, row_tap, col_tap], preferred_element_type=jnp.float32)
        return summed.reshape(height, breadth, -1)
    return lax.map(one_frame, jnp.arange(frames, dtype=jnp.int32))

def butterfly(blocks, which_axis):
    leading = lax.index_in_dim(blocks, 0, which_axis, keepdims=False)
    trailing = lax.index_in_dim(blocks, 1, which_axis, keepdims=False)
    return (leading + trailing, leading - trailing)

def haar_project(level_two, down_weight):
    frames, height, breadth, channels = level_two.shape
    blocks = level_two.astype(jnp.float32).reshape(frames // 2, 2, height // 2, 2, breadth // 2, 2, channels)
    projected = jnp.zeros((frames // 2 * (height // 2) * (breadth // 2), down_weight.shape[-1]), jnp.float32)
    band_index = 0
    for time_part in butterfly(blocks, 1):
        for row_part in butterfly(time_part, 2):
            for col_part in butterfly(row_part, 3):
                subband = (col_part * haar_scale).astype(jnp.bfloat16).reshape(-1, channels)
                projected = projected + jnp.dot(subband, down_weight[band_index], preferred_element_type=jnp.float32)
                band_index = band_index + 1
    return projected.reshape(frames // 2, height // 2, breadth // 2, -1)

def reference(feat_mid, gain_mid, conv_mid, down_weight, wavelets, inject_weight, gain_deep, conv_deep):
    normed_mid = norm_act(feat_mid.astype(jnp.float32), gain_mid)
    conv_mid_out = causal_conv(normed_mid, conv_mid)
    level_two = (feat_mid.astype(jnp.float32) + conv_mid_out).astype(jnp.bfloat16)
    frames, height, breadth, channels = level_two.shape
    frame_pairs = level_two.reshape(frames // 2, 2, height, breadth, channels)

    def deep_frame(operands):
        frame_pair, coefficients = operands
        injected = jnp.einsum('bhw,bd->hwd', coefficients.astype(jnp.float32), inject_weight.astype(jnp.float32), precision=lax.Precision.HIGHEST)
        return haar_project(frame_pair, down_weight)[0] + injected
    feat_deep = lax.map(deep_frame, (frame_pairs, wavelets))
    normed_deep = norm_act(feat_deep, gain_deep)
    conv_deep_out = causal_conv(normed_deep, conv_deep)
    return (feat_deep + conv_deep_out).astype(jnp.bfloat16)
```

```python
import functools
import jax
import jax.numpy as jnp
from jax import lax
from jax.experimental import pallas as pl
from jax.experimental.pallas import tpu as pltpu
from jax.sharding import PartitionSpec as P

epsilon = 1e-06
haar_scale = 0.35355339059327373
PAD = 8
MIB = 1 << 20


def vmem():
    return pl.BlockSpec(memory_space=pltpu.VMEM)


def call(kernel, outs, ins, scratch=(), flops=0, limit=24, aliases=None):
    bytes_accessed = sum(int(a.size) * a.dtype.itemsize for a in ins)
    return pl.pallas_call(
        kernel,
        out_shape=outs,
        in_specs=[vmem() for _ in ins],
        out_specs=jax.tree.map(lambda _: vmem(), outs),
        scratch_shapes=list(scratch),
        input_output_aliases=aliases or {},
        compiler_params=pltpu.CompilerParams(vmem_limit_bytes=limit * MIB),
        cost_estimate=pl.CostEstimate(
            flops=int(flops), bytes_accessed=bytes_accessed, transcendentals=0
        ),
    )(*ins)


def norm_act(values, gain):
    average = jnp.mean(values, axis=-1, keepdims=True)
    centred = values - average
    spread = jnp.mean(centred * centred, axis=-1, keepdims=True)
    u = centred * lax.rsqrt(spread + epsilon) * gain
    return (u * (0.5 * jnp.tanh(0.5 * u) + 0.5)).astype(jnp.bfloat16)


def norm_kernel(feat_ref, gain_ref, down_ref, x_ref, v_ref, *, step):
    frames, height, width, channels = feat_ref.shape
    gain = gain_ref[...]

    def body(index, carry):
        f = index // (height // step)
        h = (index % (height // step)) * step
        values = feat_ref[f, pl.ds(h, step)].reshape(step * width, channels)
        x_ref[f, pl.ds(h + 1, step)] = norm_act(values.astype(jnp.float32), gain).reshape(
            step, width, channels
        )
        return carry

    lax.fori_loop(0, frames * height // step, body, 0)

    rows = 16

    def fold(index, carry):
        r = pl.multiple_of(index * rows, rows)
        parts = [down_ref[s, pl.ds(r, rows), :].astype(jnp.float32) for s in range(8)]
        for bit in (4, 2, 1):
            parts = [
                parts[s] + parts[s + bit] if not s & bit else parts[s - bit] - parts[s]
                for s in range(8)
            ]
        for s in range(8):
            v_ref[s, pl.ds(r, rows), :] = (parts[s] * haar_scale).astype(jnp.bfloat16)
        return carry

    lax.fori_loop(0, channels // rows, fold, 0)


def conv_pair(pair, x_ref, w_ref, feat_ref, v_ref, y_ref, lev_ref):
    frames, ext, width, channels = x_ref.shape
    half = width // 2
    deep_rows = (ext - 2) // 2
    zero_pad = jnp.zeros((PAD, y_ref.shape[-1]), jnp.float32)
    for i in range(2):
        for j in range(2):
            for q in range(y_ref.shape[3]):
                y_ref[i, 0, j, q, 0:PAD, :] = zero_pad
                y_ref[i, 2, j, q, PAD + width : 2 * PAD + width, :] = zero_pad

    def body(h2, carry):
        for i in range(2):
            f = 2 * pair + i
            taps = [a for a in range(3) if 0 <= f + a - 2 < frames]
            for c in range(3):
                total = None
                for a in taps:
                    for b in range(3):
                        rows = x_ref[f + a - 2, pl.ds(2 * h2 + b, 2)].reshape(2 * width, channels)
                        part = jnp.dot(
                            rows, w_ref[a, b, c], preferred_element_type=jnp.float32
                        )
                        total = part if total is None else total + part
                if c == 1 and feat_ref is not None:
                    total = total + feat_ref[f, pl.ds(2 * h2, 2)].reshape(
                        2 * width, channels
                    ).astype(jnp.float32)
                for j in range(2):
                    for q in range(channels // 128):
                        y_ref[i, c, j, q, PAD : PAD + width, :] = total[
                            j * width : (j + 1) * width, q * 128 : (q + 1) * 128
                        ]
            for j in range(2):
                for k in range(2):
                    for q in range(channels // 128):
                        level = None
                        for c in range(3):
                            piece = y_ref[i, c, j, q, pl.ds(PAD + k + c - 1, half, stride=2), :]
                            level = piece if level is None else level + piece
                        lev_ref[4 * i + 2 * j + k, h2, :, q * 128 : (q + 1) * 128] = level.astype(
                            jnp.bfloat16
                        )
        return carry

    lax.fori_loop(0, deep_rows, body, 0)
    total = None
    for s in range(8):
        part = jnp.dot(
            lev_ref[s].reshape(deep_rows * half, channels),
            v_ref[s],
            preferred_element_type=jnp.float32,
        )
        total = part if total is None else total + part
    return total


def carry_kernel(x_in, up_ref, down_ref, gain_ref, w_ref, v_ref, x_ref, out_ref, y_ref, lev_ref):
    frames, ext, width, channels = x_ref.shape
    gain = gain_ref[...]
    for f in range(frames):
        x_ref[f, 0] = norm_act(up_ref[f, 0].astype(jnp.float32), gain)
        x_ref[f, ext - 1] = norm_act(down_ref[f, 0].astype(jnp.float32), gain)
    projected = conv_pair(frames // 2, x_ref, w_ref, None, v_ref, y_ref, lev_ref)
    out_ref[...] = projected.reshape(out_ref.shape).astype(out_ref.dtype)


def own_kernel(*refs, pair, extra):
    x_ref, feat_ref, w_ref, v_ref, wav_ref, inj_ref, gain_ref = refs[:7]
    carried_ref = refs[7] if extra else None
    deep_ref, normed_ref, y_ref, lev_ref = refs[7 + extra :]
    value = conv_pair(pair, x_ref, w_ref, feat_ref, v_ref, y_ref, lev_ref)
    value = value + jnp.dot(wav_ref[pair], inj_ref[...], preferred_element_type=jnp.float32)
    if extra:
        value = value + carried_ref[...].reshape(value.shape).astype(jnp.float32)
    deep_ref[...] = value.reshape(deep_ref.shape)
    normed_ref[...] = norm_act(value, gain_ref[...]).reshape(normed_ref.shape)


def deep_conv(targets, ext_ref, w_ref, z_ref):
    frames, ext, width, channels = ext_ref.shape
    rows = ext - 2
    results = []
    for target in targets:
        for c in range(3):
            total = None
            for a in range(3):
                source = target + a - 2
                if 0 <= source < frames:
                    for b in range(3):
                        part = jnp.dot(
                            ext_ref[source, b : b + rows].reshape(rows * width, channels),
                            w_ref[a, b, c],
                            preferred_element_type=jnp.float32,
                        )
                        total = part if total is None else total + part
            z_ref[c, :, PAD : PAD + width, :] = total.reshape(rows, width, -1)
        results.append(
            z_ref[0, :, PAD - 1 : PAD - 1 + width, :]
            + z_ref[1, :, PAD : PAD + width, :]
            + z_ref[2, :, PAD + 1 : PAD + 1 + width, :]
        )
        yield target, results[-1]


def fill_ext(ext_ref, own_refs, up_ref, down_ref, z_ref):
    frames, ext, width, channels = ext_ref.shape
    for f in range(frames):
        ext_ref[f, 0] = up_ref[f, 0]
        ext_ref[f, 1 : ext - 1] = own_refs[f][...]
        ext_ref[f, ext - 1] = down_ref[f, 0]
    zero_pad = jnp.zeros((ext - 2, PAD, z_ref.shape[-1]), jnp.float32)
    z_ref[0, :, 0:PAD, :] = zero_pad
    z_ref[2, :, PAD + width : 2 * PAD + width, :] = zero_pad


def deep_carry_kernel(*refs, frames):
    own_refs = refs[:frames]
    up_ref, down_ref, w_ref, out_ref, ext_ref, z_ref = refs[frames:]
    fill_ext(ext_ref, own_refs, up_ref, down_ref, z_ref)
    for target, value in deep_conv(range(frames, frames + 2), ext_ref, w_ref, z_ref):
        out_ref[target - frames] = value.astype(out_ref.dtype)


def deep_own_kernel(*refs, frames):
    own_refs = refs[:frames]
    feat_refs = refs[frames : 2 * frames]
    up_ref, down_ref, w_ref, out_ref, ext_ref, z_ref = refs[2 * frames :]
    fill_ext(ext_ref, own_refs, up_ref, down_ref, z_ref)
    for target, value in deep_conv(range(frames), ext_ref, w_ref, z_ref):
        out_ref[target] = value + feat_refs[target][...]


def join_kernel(own_ref, carried_ref, out_ref):
    out_ref[...] = own_ref[...].astype(out_ref.dtype)
    out_ref[0:2] = (own_ref[0:2] + carried_ref[...].astype(jnp.float32)).astype(out_ref.dtype)


def chain(axis, step):
    count = lax.axis_size(axis)
    return [(i, i + step) for i in range(count) if 0 <= i + step < count]


def on_device(
    feat_mid, gain_mid, conv_mid, down_weight, wavelets, inject_weight, gain_deep, conv_deep
):
    frames, height, width, channels = feat_mid.shape
    deep_channels = down_weight.shape[-1]
    deep_frames, deep_rows, half = frames // 2, height // 2, width // 2
    bands = wavelets.shape[1]
    bf16, f32 = jnp.bfloat16, jnp.float32
    shape = jax.ShapeDtypeStruct
    gain_mid = gain_mid.reshape(1, -1)
    gain_deep = gain_deep.reshape(1, -1)

    up = lax.ppermute(feat_mid[:, height - 1 :], "rows", chain("rows", 1))
    down = lax.ppermute(feat_mid[:, :1], "rows", chain("rows", -1))

    wav = wavelets.transpose(0, 2, 3, 1).reshape(deep_frames, deep_rows * half, bands)
    x_shape = shape((frames, height + 2, width, channels), bf16)
    x, folded = call(
        functools.partial(norm_kernel, step=4),
        (x_shape, shape(down_weight.shape, bf16)),
        (feat_mid, gain_mid, down_weight),
        flops=5e9,
    )
    y = pltpu.VMEM((2, 3, 2, channels // 128, width + 2 * PAD, 128), f32)
    lev = pltpu.VMEM((8, deep_rows, half, channels), bf16)
    tap = 2 * height * width * channels * channels * 9
    proj = 2 * deep_rows * half * 8 * channels * deep_channels

    x, carry = call(
        carry_kernel,
        (x_shape, shape((deep_rows, half, deep_channels), bf16)),
        (x, up, down, gain_mid, conv_mid, folded),
        (y, lev),
        flops=3 * tap + proj,
        aliases={0: 0},
    )
    carried = lax.ppermute(carry, "tm", chain("tm", 1))
    deep, normed = [None] * deep_frames, [None] * deep_frames
    for pair in reversed(range(deep_frames)):
        extra = pair == 0
        deep[pair], normed[pair] = call(
            functools.partial(own_kernel, pair=pair, extra=extra),
            (
                shape((deep_rows, half, deep_channels), f32),
                shape((deep_rows, half, deep_channels), bf16),
            ),
            (x, feat_mid, conv_mid, folded, wav, inject_weight, gain_deep)
            + ((carried,) if extra else ()),
            (y, lev),
            flops=(3 if extra else 6) * tap + proj,
        )
    up = lax.ppermute(
        jnp.stack([n[deep_rows - 1 :] for n in normed]), "rows", chain("rows", 1)
    )
    down = lax.ppermute(jnp.stack([n[:1] for n in normed]), "rows", chain("rows", -1))
    ext = pltpu.VMEM((deep_frames, deep_rows + 2, half, deep_channels), bf16)
    z = pltpu.VMEM((3, deep_rows, half + 2 * PAD, deep_channels), f32)
    tap = 2 * deep_rows * half * deep_channels * deep_channels * 9
    carry = call(
        functools.partial(deep_carry_kernel, frames=deep_frames),
        shape((2, deep_rows, half, deep_channels), bf16),
        (*normed, up, down, conv_deep),
        (ext, z),
        flops=3 * tap,
    )
    carried = lax.ppermute(carry, "tm", chain("tm", 1))
    own = call(
        functools.partial(deep_own_kernel, frames=deep_frames),
        shape((deep_frames, deep_rows, half, deep_channels), f32),
        (*normed, *deep, up, down, conv_deep),
        (ext, z),
        flops=(3 * deep_frames - 3) * tap,
    )
    return call(
        join_kernel,
        shape((deep_frames, deep_rows, half, deep_channels), bf16),
        (own, carried),
    )


def solution(mesh):
    return jax.shard_map(
        on_device,
        mesh=mesh,
        in_specs=(
            P("tm", "rows", None, None),
            P(),
            P(),
            P(),
            P("tm", None, "rows", None),
            P(),
            P(),
            P(),
        ),
        out_specs=P("tm", "rows", None, None),
        check_vma=False,
    )
```

```python
import functools
import jax
import jax.numpy as jnp
from jax import lax
from jax.experimental import pallas as pl
from jax.experimental.pallas import tpu as pltpu
from jax.sharding import PartitionSpec as P

epsilon = 1e-06
haar_scale = 0.35355339059327373
PAD = 8
MIB = 1 << 20


def vmem():
    return pl.BlockSpec(memory_space=pltpu.VMEM)


def call(kernel, outs, ins, scratch=(), flops=0, limit=14, aliases=None, hbm=()):
    bytes_accessed = sum(int(a.size) * a.dtype.itemsize for a in ins)
    ins = [
        pltpu.with_memory_space_constraint(a, pltpu.HBM) if n in hbm else a
        for n, a in enumerate(ins)
    ]
    return pl.pallas_call(
        kernel,
        out_shape=outs,
        in_specs=[
            pl.BlockSpec(memory_space=pltpu.HBM) if n in hbm else vmem()
            for n in range(len(ins))
        ],
        out_specs=tuple(vmem() for _ in outs) if isinstance(outs, tuple) else vmem(),
        scratch_shapes=list(scratch),
        input_output_aliases=aliases or {},
        compiler_params=pltpu.CompilerParams(vmem_limit_bytes=limit * MIB),
        cost_estimate=pl.CostEstimate(
            flops=int(flops), bytes_accessed=bytes_accessed, transcendentals=0
        ),
    )(*ins)


def norm_act(values, gain):
    average = jnp.mean(values, axis=-1, keepdims=True)
    centred = values - average
    spread = jnp.mean(centred * centred, axis=-1, keepdims=True)
    u = centred * lax.rsqrt(spread + epsilon) * gain
    return u * (0.5 * jnp.tanh(0.5 * u) + 0.5)


def haar_cols(raw_ref, half):
    even = [raw_ref[:, q, pl.ds(0, half, stride=2), :] for q in range(raw_ref.shape[1])]
    odd = [raw_ref[:, q, pl.ds(1, half, stride=2), :] for q in range(raw_ref.shape[1])]
    return jnp.concatenate(even, -1), jnp.concatenate(odd, -1)


def prepare(values, gain, raw_ref, pad_ref, store, residual=None):
    rows, width, channels = values.shape
    half = width // 2
    for q in range(channels // 128):
        raw_ref[:, q] = values[:, :, q * 128 : (q + 1) * 128].astype(jnp.float32)
    even, odd = haar_cols(raw_ref, half)
    if residual is not None:
        residual(0, even + odd)
        residual(1, even - odd)
    even, odd = norm_act(even, gain), norm_act(odd, gain)
    pad_ref[0, :, PAD : PAD + half, :] = odd
    pad_ref[1, :, PAD : PAD + half, :] = even
    store(0, pad_ref[0, :, PAD - 1 : PAD - 1 + half, :] - odd)
    store(1, even + odd)
    store(2, odd - even)
    store(3, even - pad_ref[1, :, PAD + 1 : PAD + 1 + half, :])


def clear_pads(pad_ref):
    rows, ext, channels = pad_ref.shape[1:]
    zero = jnp.zeros((rows, PAD, channels), jnp.float32)
    pad_ref[0, :, 0:PAD, :] = zero
    pad_ref[1, :, ext - PAD :, :] = zero


def norm_kernel(
    feat_hbm, gain_hbm, down_hbm, w_hbm, x_ref, res_ref, v_ref, g_ref,
    feat_ref, gain_ref, down_ref, w_ref, raw_ref, pad_ref, feat_sem, gain_sem, down_sem, w_sem,
    *, step
):
    frames, height, width, channels = feat_ref.shape
    half = width // 2
    feat_copies = [
        pltpu.make_async_copy(feat_hbm.at[f], feat_ref.at[f], feat_sem.at[f])
        for f in range(frames)
    ]
    w_copies = [pltpu.make_async_copy(w_hbm.at[a], w_ref.at[a], w_sem.at[a]) for a in range(3)]
    down_copy = pltpu.make_async_copy(down_hbm, down_ref, down_sem)
    gain_copy = pltpu.make_async_copy(gain_hbm, gain_ref, gain_sem)
    for copy in (gain_copy, *feat_copies, *w_copies, down_copy):
        copy.start()
    clear_pads(pad_ref)
    gain_copy.wait()
    gain = gain_ref[...]

    for f in range(frames):
        feat_copies[f].wait()

        def body(index, carry):
            h = index * step

            def store(t, value):
                x_ref[f, t, pl.ds(h + 1, step)] = value.astype(jnp.bfloat16)

            def residual(r, value):
                res_ref[f, r, pl.ds(h, step)] = value

            prepare(feat_ref[f, pl.ds(h, step)], gain, raw_ref, pad_ref, store, residual)
            return carry

        lax.fori_loop(0, height // step, body, 0)

    for a in range(3):
        w_copies[a].wait()

        def combine(b, carry):
            first, mid, last = (w_ref[a, b, c].astype(jnp.float32) for c in range(3))
            outer = first + last
            g_ref[a, b, 0] = (outer + mid).astype(jnp.bfloat16)
            g_ref[a, b, 1] = (outer - mid).astype(jnp.bfloat16)
            return carry

        lax.fori_loop(0, 3, combine, 0)

    down_copy.wait()
    rows = 32

    def fold(index, carry):
        r = pl.multiple_of(index * rows, rows)
        parts = [down_ref[s, pl.ds(r, rows), :].astype(jnp.float32) for s in range(8)]
        for bit in (4, 2):
            parts = [
                parts[s] + parts[s + bit] if not s & bit else parts[s - bit] - parts[s]
                for s in range(8)
            ]
        for s in range(8):
            v_ref[s, pl.ds(r, rows), :] = (parts[s] * haar_scale).astype(jnp.bfloat16)
        return carry

    lax.fori_loop(0, channels // rows, fold, 0)


def conv_pair(pair, x_ref, w_ref, g_ref, res_ref, v_ref, lev_ref, group):
    frames, _, ext, half, channels = x_ref.shape
    deep_rows = (ext - 2) // 2

    def body(index, carry):
        start = 2 * group * index
        for i in range(2):
            f = 2 * pair + i
            taps = [a for a in range(3) if 0 <= f + a - 2 < frames]
            sums = []
            for t in range(4):
                total = None
                for a in taps:
                    for b in range(3):
                        rows = x_ref[f + a - 2, t, pl.ds(start + b, 2 * group)].reshape(
                            2 * group * half, channels
                        )
                        weight = (
                            w_ref[a, b, 0], g_ref[a, b, 0], g_ref[a, b, 1], w_ref[a, b, 2]
                        )[t]
                        part = jnp.dot(rows, weight, preferred_element_type=jnp.float32)
                        total = part if total is None else total + part
                sums.append(total)
            pieces = (sums[0] - sums[3] + sums[1], sums[0] + sums[3] + sums[2])
            for r in range(2):
                level = pieces[r].reshape(2 * group, half, channels)
                if res_ref is not None:
                    level = level + res_ref[f, r, pl.ds(start, 2 * group)]
                level = level.astype(jnp.bfloat16)
                for row in range(2 * group):
                    lev_ref[4 * i + 2 * (row % 2) + r, index * group + row // 2] = level[row]
        return carry

    lax.fori_loop(0, deep_rows // group, body, 0)
    total = None
    for s in range(8):
        part = jnp.dot(
            lev_ref[s].reshape(deep_rows * half, channels),
            v_ref[s],
            preferred_element_type=jnp.float32,
        )
        total = part if total is None else total + part
    return total


def carry_kernel(
    x_in, near_ref, far_ref, gain_ref, w_ref, g_ref, v_ref, x_ref, out_ref,
    lev_ref, raw_ref, pad_ref, *, group
):
    frames, _, ext, half, channels = x_ref.shape
    gain = gain_ref[...]
    odd = lax.rem(lax.axis_index("rows"), 2)
    clear_pads(pad_ref)
    for ref, row in ((near_ref, (1 - odd) * (ext - 1)), (far_ref, odd * (ext - 1))):

        def store(t, value):
            for f in range(frames):
                x_ref[f, t, row] = value[f].astype(jnp.bfloat16)

        prepare(ref[:, 0], gain, raw_ref, pad_ref, store)
    projected = conv_pair(frames // 2, x_ref, w_ref, g_ref, None, v_ref, lev_ref, group)
    out_ref[...] = projected.reshape(out_ref.shape).astype(out_ref.dtype)


def own_kernel(*refs, pair, extra, group):
    x_ref, res_ref, w_ref, g_ref, v_ref, wav_ref, inj_ref, gain_ref = refs[:8]
    carried_ref = refs[8] if extra else None
    deep_ref, normed_ref, lev_ref = refs[8 + extra :]
    value = conv_pair(pair, x_ref, w_ref, g_ref, res_ref, v_ref, lev_ref, group)
    value = value + jnp.dot(wav_ref[pair], inj_ref[...], preferred_element_type=jnp.float32)
    if extra:
        value = value + carried_ref[...].reshape(value.shape).astype(jnp.float32)
    deep_ref[...] = value.reshape(deep_ref.shape)
    normed_ref[...] = norm_act(value, gain_ref[...]).reshape(normed_ref.shape).astype(
        normed_ref.dtype
    )


def deep_conv(targets, ext_ref, w_ref, z_ref):
    frames, ext, width, channels = ext_ref.shape
    rows = ext - 2
    results = []
    for target in targets:
        for c in range(3):
            total = None
            for a in range(3):
                source = target + a - 2
                if 0 <= source < frames:
                    for b in range(3):
                        part = jnp.dot(
                            ext_ref[source, b : b + rows].reshape(rows * width, channels),
                            w_ref[a, b, c],
                            preferred_element_type=jnp.float32,
                        )
                        total = part if total is None else total + part
            z_ref[c, :, PAD : PAD + width, :] = total.reshape(rows, width, -1)
        results.append(
            z_ref[0, :, PAD - 1 : PAD - 1 + width, :]
            + z_ref[1, :, PAD : PAD + width, :]
            + z_ref[2, :, PAD + 1 : PAD + 1 + width, :]
        )
        yield target, results[-1]


def fill_ext(ext_ref, own_refs, near_ref, far_ref, z_ref):
    frames, ext, width, channels = ext_ref.shape
    odd = lax.rem(lax.axis_index("rows"), 2)
    for f in range(frames):
        ext_ref[f, 1 : ext - 1] = own_refs[f][...]
        ext_ref[f, (1 - odd) * (ext - 1)] = near_ref[f, 0]
        ext_ref[f, odd * (ext - 1)] = far_ref[f, 0]
    zero_pad = jnp.zeros((ext - 2, PAD, z_ref.shape[-1]), jnp.float32)
    z_ref[0, :, 0:PAD, :] = zero_pad
    z_ref[2, :, PAD + width : 2 * PAD + width, :] = zero_pad


def deep_carry_kernel(*refs, frames):
    own_refs = refs[:frames]
    near_ref, far_ref, w_ref, out_ref, ext_ref, z_ref = refs[frames:]
    fill_ext(ext_ref, own_refs, near_ref, far_ref, z_ref)
    for target, value in deep_conv(range(frames, frames + 2), ext_ref, w_ref, z_ref):
        out_ref[target - frames] = value.astype(out_ref.dtype)


def deep_own_kernel(*refs, frames):
    own_refs = refs[:frames]
    feat_refs = refs[frames : 2 * frames]
    near_ref, far_ref, w_ref, out_ref, ext_ref, z_ref = refs[2 * frames :]
    fill_ext(ext_ref, own_refs, near_ref, far_ref, z_ref)
    for target, value in deep_conv(range(frames), ext_ref, w_ref, z_ref):
        out_ref[target] = value + feat_refs[target][...]


def join_kernel(own_ref, carried_ref, out_ref):
    out_ref[...] = own_ref[...].astype(out_ref.dtype)
    out_ref[0:2] = (own_ref[0:2] + carried_ref[...].astype(jnp.float32)).astype(out_ref.dtype)


def chain(axis, step):
    count = lax.axis_size(axis)
    return [(i, i + step) for i in range(count) if 0 <= i + step < count]


def exchange(first_rows, last_rows):
    odd = lax.rem(lax.axis_index("rows"), 2) == 1
    count = lax.axis_size("rows")
    routes = [
        [(i + x, i + 1 - x) for i in range(first, count - 1, 2) for x in range(2)]
        for first in range(2)
    ]
    far = lax.ppermute(jnp.where(odd, last_rows, first_rows), "rows", routes[1])
    near = lax.ppermute(jnp.where(odd, first_rows, last_rows), "rows", routes[0])
    return near, far


def on_device(
    feat_mid, gain_mid, conv_mid, down_weight, wavelets, inject_weight, gain_deep, conv_deep
):
    frames, height, width, channels = feat_mid.shape
    deep_channels = down_weight.shape[-1]
    deep_frames, deep_rows, half = frames // 2, height // 2, width // 2
    bands = wavelets.shape[1]
    group = 2 if deep_rows % 2 == 0 else 1
    bf16, f32 = jnp.bfloat16, jnp.float32
    shape = jax.ShapeDtypeStruct
    local = pltpu.VMEM
    gain_mid = gain_mid.reshape(1, -1)
    gain_deep = gain_deep.reshape(1, -1)

    near, far = exchange(feat_mid[:, :1], feat_mid[:, height - 1 :])
    wav = wavelets.transpose(0, 2, 3, 1).reshape(deep_frames, deep_rows * half, bands)
    x_shape = local((frames, 4, height + 2, half, channels), bf16)
    step = 4
    sem = pltpu.SemaphoreType.DMA
    x, residual, folded, mixed = call(
        functools.partial(norm_kernel, step=step),
        (
            x_shape,
            local((frames, 2, height, half, channels), f32),
            local(down_weight.shape, bf16),
            local((3, 3, 2) + conv_mid.shape[-2:], bf16),
        ),
        (feat_mid, gain_mid, down_weight, conv_mid),
        (
            pltpu.VMEM(feat_mid.shape, bf16),
            pltpu.VMEM(gain_mid.shape, f32),
            pltpu.VMEM(down_weight.shape, bf16),
            pltpu.VMEM(conv_mid.shape, bf16),
            pltpu.VMEM((step, channels // 128, width, 128), f32),
            pltpu.VMEM((2, step, half + 2 * PAD, channels), f32),
            sem((frames,)),
            sem(()),
            sem(()),
            sem((3,)),
        ),
        flops=5e9,
        hbm=(0, 1, 2, 3),
    )
    lev = pltpu.VMEM((8, deep_rows, half, channels), bf16)
    tap = 2 * height * width * channels * channels * 6
    proj = 2 * deep_rows * half * 8 * channels * deep_channels

    x, carry = call(
        functools.partial(carry_kernel, group=group),
        (x_shape, shape((deep_rows, half, deep_channels), bf16)),
        (x, near, far, gain_mid, conv_mid, mixed, folded),
        (
            lev,
            pltpu.VMEM((frames, channels // 128, width, 128), f32),
            pltpu.VMEM((2, frames, half + 2 * PAD, channels), f32),
        ),
        flops=3 * tap + proj,
        aliases={0: 0},
    )
    carried = lax.ppermute(carry, "tm", chain("tm", 1))
    deep, normed = [None] * deep_frames, [None] * deep_frames
    for pair in reversed(range(deep_frames)):
        extra = pair == 0
        deep[pair], normed[pair] = call(
            functools.partial(own_kernel, pair=pair, extra=extra, group=group),
            (
                shape((deep_rows, half, deep_channels), f32),
                shape((deep_rows, half, deep_channels), bf16),
            ),
            (x, residual, conv_mid, mixed, folded, wav, inject_weight, gain_deep)
            + ((carried,) if extra else ()),
            (lev,),
            flops=(3 if extra else 6) * tap + proj,
        )
    near, far = exchange(
        jnp.stack([n[:1] for n in normed]), jnp.stack([n[deep_rows - 1 :] for n in normed])
    )
    ext = pltpu.VMEM((deep_frames, deep_rows + 2, half, deep_channels), bf16)
    z = pltpu.VMEM((3, deep_rows, half + 2 * PAD, deep_channels), f32)
    tap = 2 * deep_rows * half * deep_channels * deep_channels * 9
    carry = call(
        functools.partial(deep_carry_kernel, frames=deep_frames),
        shape((2, deep_rows, half, deep_channels), bf16),
        (*normed, near, far, conv_deep),
        (ext, z),
        flops=3 * tap,
    )
    carried = lax.ppermute(carry, "tm", chain("tm", 1))
    own = call(
        functools.partial(deep_own_kernel, frames=deep_frames),
        shape((deep_frames, deep_rows, half, deep_channels), f32),
        (*normed, *deep, near, far, conv_deep),
        (ext, z),
        flops=(3 * deep_frames - 3) * tap,
    )
    return call(
        join_kernel,
        shape((deep_frames, deep_rows, half, deep_channels), bf16),
        (own, carried),
    )


def solution(mesh):
    return jax.shard_map(
        on_device,
        mesh=mesh,
        in_specs=(
            P("tm", "rows", None, None),
            P(),
            P(),
            P(),
            P("tm", None, "rows", None),
            P(),
            P(),
            P(),
        ),
        out_specs=P("tm", "rows", None, None),
        check_vma=False,
    )
```

```python
import functools
import jax
import jax.numpy as jnp
from jax import lax
from jax.experimental import pallas as pl
from jax.experimental.pallas import tpu as pltpu
from jax.sharding import PartitionSpec as P

epsilon = 1e-06
haar_scale = 0.35355339059327373
PAD = 8
MIB = 1 << 20


def vmem():
    return pl.BlockSpec(memory_space=pltpu.VMEM)


def call(kernel, outs, ins, scratch=(), flops=0, limit=14, aliases=None, hbm=()):
    bytes_accessed = sum(int(a.size) * a.dtype.itemsize for a in ins)
    ins = [
        pltpu.with_memory_space_constraint(a, pltpu.HBM) if n in hbm else a
        for n, a in enumerate(ins)
    ]
    return pl.pallas_call(
        kernel,
        out_shape=outs,
        in_specs=[
            pl.BlockSpec(memory_space=pltpu.HBM) if n in hbm else vmem()
            for n in range(len(ins))
        ],
        out_specs=tuple(vmem() for _ in outs) if isinstance(outs, tuple) else vmem(),
        scratch_shapes=list(scratch),
        input_output_aliases=aliases or {},
        compiler_params=pltpu.CompilerParams(vmem_limit_bytes=limit * MIB),
        cost_estimate=pl.CostEstimate(
            flops=int(flops), bytes_accessed=bytes_accessed, transcendentals=0
        ),
    )(*ins)


def norm_act(values, gain):
    average = jnp.mean(values, axis=-1, keepdims=True)
    centred = values - average
    spread = jnp.mean(centred * centred, axis=-1, keepdims=True)
    u = centred * lax.rsqrt(spread + epsilon) * gain
    return u * (0.5 * jnp.tanh(0.5 * u) + 0.5)


def haar_cols(raw_ref, half):
    even = [raw_ref[:, q, pl.ds(0, half, stride=2), :] for q in range(raw_ref.shape[1])]
    odd = [raw_ref[:, q, pl.ds(1, half, stride=2), :] for q in range(raw_ref.shape[1])]
    return jnp.concatenate(even, -1), jnp.concatenate(odd, -1)


def prepare(values, gain, raw_ref, pad_ref, store, residual=None):
    rows, width, channels = values.shape
    half = width // 2
    for q in range(channels // 128):
        raw_ref[:, q] = values[:, :, q * 128 : (q + 1) * 128].astype(jnp.float32)
    even, odd = haar_cols(raw_ref, half)
    if residual is not None:
        residual(0, even + odd)
        residual(1, even - odd)
    even, odd = norm_act(even, gain), norm_act(odd, gain)
    pad_ref[0, :, PAD : PAD + half, :] = odd
    pad_ref[1, :, PAD : PAD + half, :] = even
    store(0, pad_ref[0, :, PAD - 1 : PAD - 1 + half, :] - odd)
    store(1, even + odd)
    store(2, odd - even)
    store(3, even - pad_ref[1, :, PAD + 1 : PAD + 1 + half, :])


def clear_pads(pad_ref):
    rows, ext, channels = pad_ref.shape[1:]
    zero = jnp.zeros((rows, PAD, channels), jnp.float32)
    pad_ref[0, :, 0:PAD, :] = zero
    pad_ref[1, :, ext - PAD :, :] = zero


def norm_kernel(
    feat_hbm, gain_hbm, down_hbm, w_hbm, x_ref, res_ref, v_ref, g_ref,
    feat_ref, gain_ref, down_ref, w_ref, raw_ref, pad_ref, feat_sem, gain_sem, down_sem, w_sem,
    *, step
):
    frames, height, width, channels = feat_ref.shape
    half = width // 2
    feat_copies = [
        pltpu.make_async_copy(feat_hbm.at[f], feat_ref.at[f], feat_sem.at[f])
        for f in range(frames)
    ]
    w_copies = [pltpu.make_async_copy(w_hbm.at[a], w_ref.at[a], w_sem.at[a]) for a in range(3)]
    down_copy = pltpu.make_async_copy(down_hbm, down_ref, down_sem)
    gain_copy = pltpu.make_async_copy(gain_hbm, gain_ref, gain_sem)
    for copy in (gain_copy, *feat_copies, *w_copies, down_copy):
        copy.start()
    clear_pads(pad_ref)
    gain_copy.wait()
    gain = gain_ref[...]

    for f in range(frames):
        feat_copies[f].wait()

        def body(index, carry):
            h = index * step

            def store(t, value):
                x_ref[f, t, pl.ds(h + 1, step)] = value.astype(jnp.bfloat16)

            def residual(r, value):
                res_ref[f, r, pl.ds(h, step)] = value

            prepare(feat_ref[f, pl.ds(h, step)], gain, raw_ref, pad_ref, store, residual)
            return carry

        lax.fori_loop(0, height // step, body, 0)

    for a in range(3):
        w_copies[a].wait()

        def combine(b, carry):
            first, mid, last = (w_ref[a, b, c].astype(jnp.float32) for c in range(3))
            outer = first + last
            g_ref[a, b, 0] = (outer + mid).astype(jnp.bfloat16)
            g_ref[a, b, 1] = (outer - mid).astype(jnp.bfloat16)
            return carry

        lax.fori_loop(0, 3, combine, 0)

    down_copy.wait()
    rows = 32

    def fold(index, carry):
        r = pl.multiple_of(index * rows, rows)
        parts = [down_ref[s, pl.ds(r, rows), :].astype(jnp.float32) for s in range(8)]
        for bit in (4, 2):
            parts = [
                parts[s] + parts[s + bit] if not s & bit else parts[s - bit] - parts[s]
                for s in range(8)
            ]
        for s in range(8):
            v_ref[s, pl.ds(r, rows), :] = (parts[s] * haar_scale).astype(jnp.bfloat16)
        return carry

    lax.fori_loop(0, channels // rows, fold, 0)


def conv_pair(pair, x_ref, w_ref, g_ref, res_ref, v_ref, lev_ref, group):
    frames, _, ext, half, channels = x_ref.shape
    deep_rows = (ext - 2) // 2

    def body(index, carry):
        start = 2 * group * index
        for i in range(2):
            f = 2 * pair + i
            taps = [a for a in range(3) if 0 <= f + a - 2 < frames]
            sums = []
            for t in range(4):
                total = None
                for a in taps:
                    for b in range(3):
                        rows = x_ref[f + a - 2, t, pl.ds(start + b, 2 * group)].reshape(
                            2 * group * half, channels
                        )
                        weight = (
                            w_ref[a, b, 0], g_ref[a, b, 0], g_ref[a, b, 1], w_ref[a, b, 2]
                        )[t]
                        part = jnp.dot(rows, weight, preferred_element_type=jnp.float32)
                        total = part if total is None else total + part
                sums.append(total)
            pieces = (sums[0] - sums[3] + sums[1], sums[0] + sums[3] + sums[2])
            for r in range(2):
                level = pieces[r].reshape(2 * group, half, channels)
                if res_ref is not None:
                    level = level + res_ref[f, r, pl.ds(start, 2 * group)]
                level = level.astype(jnp.bfloat16)
                for row in range(2 * group):
                    lev_ref[4 * i + 2 * (row % 2) + r, index * group + row // 2] = level[row]
        return carry

    lax.fori_loop(0, deep_rows // group, body, 0)
    total = None
    for s in range(8):
        part = jnp.dot(
            lev_ref[s].reshape(deep_rows * half, channels),
            v_ref[s],
            preferred_element_type=jnp.float32,
        )
        total = part if total is None else total + part
    return total


def carry_kernel(
    x_in, near_ref, far_ref, gain_ref, w_ref, g_ref, v_ref, x_ref, out_ref,
    lev_ref, raw_ref, pad_ref, *, group
):
    frames, _, ext, half, channels = x_ref.shape
    gain = gain_ref[...]
    odd = lax.rem(lax.axis_index("rows"), 2)
    clear_pads(pad_ref)
    for ref, row in ((near_ref, (1 - odd) * (ext - 1)), (far_ref, odd * (ext - 1))):

        def store(t, value):
            for f in range(frames):
                x_ref[f, t, row] = value[f].astype(jnp.bfloat16)

        prepare(ref[:, 0], gain, raw_ref, pad_ref, store)
    projected = conv_pair(frames // 2, x_ref, w_ref, g_ref, None, v_ref, lev_ref, group)
    out_ref[...] = projected.reshape(out_ref.shape).astype(out_ref.dtype)


def own_kernel(*refs, pair, extra, group):
    x_ref, res_ref, w_ref, g_ref, v_ref, wav_ref, inj_ref, gain_ref = refs[:8]
    carried_ref = refs[8] if extra else None
    deep_ref, normed_ref, lev_ref = refs[8 + extra :]
    value = conv_pair(pair, x_ref, w_ref, g_ref, res_ref, v_ref, lev_ref, group)
    value = value + jnp.dot(wav_ref[pair], inj_ref[...], preferred_element_type=jnp.float32)
    if extra:
        value = value + carried_ref[...].reshape(value.shape).astype(jnp.float32)
    deep_ref[...] = value.reshape(deep_ref.shape)
    normed_ref[...] = norm_act(value, gain_ref[...]).reshape(normed_ref.shape).astype(
        normed_ref.dtype
    )


def shifted(z_ref, sums):
    rows, ext = z_ref.shape[1:3]
    width = ext - 2 * PAD
    for c in range(3):
        z_ref[c, :, PAD : PAD + width, :] = sums[c].reshape(rows, width, -1)
    return (
        z_ref[0, :, PAD - 1 : PAD - 1 + width, :]
        + z_ref[1, :, PAD : PAD + width, :]
        + z_ref[2, :, PAD + 1 : PAD + 1 + width, :]
    )


def clear_columns(z_ref):
    rows, ext, channels = z_ref.shape[1:]
    zero = jnp.zeros((rows, PAD, channels), jnp.float32)
    z_ref[0, :, 0:PAD, :] = zero
    z_ref[2, :, ext - PAD :, :] = zero


def dot(rows, weight):
    return jnp.dot(rows, weight, preferred_element_type=jnp.float32)


def deep_conv(targets, ext_ref, w_ref, z_ref):
    frames, ext, width, channels = ext_ref.shape
    rows = ext - 2
    for target in targets:
        sums = []
        for c in range(3):
            total = None
            for a in range(3):
                source = target + a - 2
                if 0 <= source < frames:
                    for b in range(3):
                        part = dot(
                            ext_ref[source, b : b + rows].reshape(rows * width, channels),
                            w_ref[a, b, c],
                        )
                        total = part if total is None else total + part
            sums.append(total)
        yield target, shifted(z_ref, sums)


def deep_carry(rows, w_ref, z_ref, out_ref):
    both, last = [], []
    for c in range(3):
        first_tap, mid_tap = None, None
        for b in range(3):
            before, latest = rows(0, b), rows(1, b)
            part = dot(jnp.concatenate([before, latest], 0), w_ref[0, b, c])
            first_tap = part if first_tap is None else first_tap + part
            part = dot(latest, w_ref[1, b, c])
            mid_tap = part if mid_tap is None else mid_tap + part
        half = mid_tap.shape[0]
        both.append(first_tap[:half] + mid_tap)
        last.append(first_tap[half:])
    out_ref[0] = shifted(z_ref, both).astype(out_ref.dtype)
    out_ref[1] = shifted(z_ref, last).astype(out_ref.dtype)


def fill_ext(ext_ref, own_refs, near_ref, far_ref):
    frames, ext, width, channels = ext_ref.shape
    odd = lax.rem(lax.axis_index("rows"), 2)
    for f in range(frames):
        ext_ref[f, 1 : ext - 1] = own_refs[f][...]
        ext_ref[f, (1 - odd) * (ext - 1)] = near_ref[f, 0]
        ext_ref[f, odd * (ext - 1)] = far_ref[f, 0]


def inner_carry_kernel(before_ref, latest_ref, w_ref, out_ref, z_ref):
    inner, ext, channels = z_ref.shape[1:]
    clear_columns(z_ref)

    def rows(f, b):
        return (before_ref, latest_ref)[f][b : b + inner].reshape(-1, channels)

    deep_carry(rows, w_ref, z_ref, out_ref)


def outer_carry_kernel(
    before_ref, latest_ref, near_ref, far_ref, w_ref, out_ref, halo_ref, z_ref
):
    count = before_ref.shape[0]
    odd = lax.rem(lax.axis_index("rows"), 2)
    clear_columns(z_ref)
    for f in range(2):
        halo_ref[f, 1 - odd] = near_ref[near_ref.shape[0] - 2 + f, 0]
        halo_ref[f, odd] = far_ref[far_ref.shape[0] - 2 + f, 0]

    def one(f, r):
        if r < 0:
            return halo_ref[f, 0]
        if r >= count:
            return halo_ref[f, 1]
        return (before_ref, latest_ref)[f][r]

    def rows(f, b):
        return jnp.concatenate([one(f, b - 1), one(f, count + b - 2)], 0)

    deep_carry(rows, w_ref, z_ref, out_ref)


def deep_own_kernel(*refs, frames):
    own_refs = refs[:frames]
    feat_refs = refs[frames : 2 * frames]
    near_ref, far_ref, w_ref, out_ref, ext_ref, z_ref = refs[2 * frames :]
    clear_columns(z_ref)
    fill_ext(ext_ref, own_refs, near_ref, far_ref)
    for target, value in deep_conv(range(frames), ext_ref, w_ref, z_ref):
        out_ref[target] = value + feat_refs[target][...]


def join_kernel(own_ref, inner_ref, outer_ref, out_ref):
    frames, rows = own_ref.shape[:2]
    for f in range(frames):
        if f < 2:
            out_ref[f, 1 : rows - 1] = (
                own_ref[f, 1 : rows - 1] + inner_ref[f].astype(jnp.float32)
            ).astype(out_ref.dtype)
            for n, r in enumerate((0, rows - 1)):
                out_ref[f, r] = (own_ref[f, r] + outer_ref[f, n].astype(jnp.float32)).astype(
                    out_ref.dtype
                )
        else:
            out_ref[f] = own_ref[f].astype(out_ref.dtype)


def chain(axis, step):
    count = lax.axis_size(axis)
    return [(i, i + step) for i in range(count) if 0 <= i + step < count]


def exchange(first_rows, last_rows):
    odd = lax.rem(lax.axis_index("rows"), 2) == 1
    count = lax.axis_size("rows")
    routes = [
        [(i + x, i + 1 - x) for i in range(first, count - 1, 2) for x in range(2)]
        for first in range(2)
    ]
    far = lax.ppermute(jnp.where(odd, last_rows, first_rows), "rows", routes[1])
    near = lax.ppermute(jnp.where(odd, first_rows, last_rows), "rows", routes[0])
    return near, far


def on_device(
    feat_mid, gain_mid, conv_mid, down_weight, wavelets, inject_weight, gain_deep, conv_deep
):
    frames, height, width, channels = feat_mid.shape
    deep_channels = down_weight.shape[-1]
    deep_frames, deep_rows, half = frames // 2, height // 2, width // 2
    bands = wavelets.shape[1]
    group = 2 if deep_rows % 2 == 0 else 1
    bf16, f32 = jnp.bfloat16, jnp.float32
    shape = jax.ShapeDtypeStruct
    local = pltpu.VMEM
    gain_mid = gain_mid.reshape(1, -1)
    gain_deep = gain_deep.reshape(1, -1)

    near, far = exchange(feat_mid[:, :1], feat_mid[:, height - 1 :])
    wav = wavelets.transpose(0, 2, 3, 1).reshape(deep_frames, deep_rows * half, bands)
    x_shape = local((frames, 4, height + 2, half, channels), bf16)
    step = 4
    sem = pltpu.SemaphoreType.DMA
    x, residual, folded, mixed = call(
        functools.partial(norm_kernel, step=step),
        (
            x_shape,
            local((frames, 2, height, half, channels), f32),
            local(down_weight.shape, bf16),
            local((3, 3, 2) + conv_mid.shape[-2:], bf16),
        ),
        (feat_mid, gain_mid, down_weight, conv_mid),
        (
            pltpu.VMEM(feat_mid.shape, bf16),
            pltpu.VMEM(gain_mid.shape, f32),
            pltpu.VMEM(down_weight.shape, bf16),
            pltpu.VMEM(conv_mid.shape, bf16),
            pltpu.VMEM((step, channels // 128, width, 128), f32),
            pltpu.VMEM((2, step, half + 2 * PAD, channels), f32),
            sem((frames,)),
            sem(()),
            sem(()),
            sem((3,)),
        ),
        flops=5e9,
        hbm=(0, 1, 2, 3),
    )
    lev = pltpu.VMEM((8, deep_rows, half, channels), bf16)
    tap = 2 * height * width * channels * channels * 6
    proj = 2 * deep_rows * half * 8 * channels * deep_channels

    x, carry = call(
        functools.partial(carry_kernel, group=group),
        (x_shape, shape((deep_rows, half, deep_channels), bf16)),
        (x, near, far, gain_mid, conv_mid, mixed, folded),
        (
            lev,
            pltpu.VMEM((frames, channels // 128, width, 128), f32),
            pltpu.VMEM((2, frames, half + 2 * PAD, channels), f32),
        ),
        flops=3 * tap + proj,
        aliases={0: 0},
    )
    carried = lax.ppermute(carry, "tm", chain("tm", 1))
    deep, normed = [None] * deep_frames, [None] * deep_frames
    for pair in reversed(range(deep_frames)):
        extra = pair == 0
        deep[pair], normed[pair] = call(
            functools.partial(own_kernel, pair=pair, extra=extra, group=group),
            (
                shape((deep_rows, half, deep_channels), f32),
                shape((deep_rows, half, deep_channels), bf16),
            ),
            (x, residual, conv_mid, mixed, folded, wav, inject_weight, gain_deep)
            + ((carried,) if extra else ()),
            (lev,),
            flops=(3 if extra else 6) * tap + proj,
        )
    near, far = exchange(
        jnp.stack([n[:1] for n in normed]), jnp.stack([n[deep_rows - 1 :] for n in normed])
    )
    ext = pltpu.VMEM((deep_frames, deep_rows + 2, half, deep_channels), bf16)
    z = pltpu.VMEM((3, deep_rows, half + 2 * PAD, deep_channels), f32)
    tap = 2 * deep_rows * half * deep_channels * deep_channels * 9
    inner_z = pltpu.VMEM((3, deep_rows - 2, half + 2 * PAD, deep_channels), f32)
    outer_z = pltpu.VMEM((3, 2, half + 2 * PAD, deep_channels), f32)
    inner = call(
        inner_carry_kernel,
        shape((2, deep_rows - 2, half, deep_channels), bf16),
        (*normed[-2:], conv_deep),
        (inner_z,),
        flops=3 * tap * (deep_rows - 2) / deep_rows,
    )
    inner = lax.ppermute(inner, "tm", chain("tm", 1))
    outer = call(
        outer_carry_kernel,
        shape((2, 2, half, deep_channels), bf16),
        (*normed[-2:], near, far, conv_deep),
        (pltpu.VMEM((2, 2, half, deep_channels), bf16), outer_z),
        flops=3 * tap * 2 / deep_rows,
    )
    outer = lax.ppermute(outer, "tm", chain("tm", 1))
    own = call(
        functools.partial(deep_own_kernel, frames=deep_frames),
        shape((deep_frames, deep_rows, half, deep_channels), f32),
        (*normed, *deep, near, far, conv_deep),
        (ext, z),
        flops=(3 * deep_frames - 3) * tap,
    )
    return call(
        join_kernel,
        shape((deep_frames, deep_rows, half, deep_channels), bf16),
        (own, inner, outer),
    )


def solution(mesh):
    return jax.shard_map(
        on_device,
        mesh=mesh,
        in_specs=(
            P("tm", "rows", None, None),
            P(),
            P(),
            P(),
            P("tm", None, "rows", None),
            P(),
            P(),
            P(),
        ),
        out_specs=P("tm", "rows", None, None),
        check_vma=False,
    )
```

```python
import functools
import jax
import jax.numpy as jnp
from jax import lax
from jax.experimental import pallas as pl
from jax.experimental.pallas import tpu as pltpu
from jax.sharding import PartitionSpec as P

epsilon = 1e-06
haar_scale = 0.35355339059327373
PAD = 8
MIB = 1 << 20
WRAPS = (1, 1, 0)


def vmem():
    return pl.BlockSpec(memory_space=pltpu.VMEM)


def call(kernel, outs, ins, scratch=(), flops=0, limit=14, aliases=None, hbm=()):
    bytes_accessed = sum(int(a.size) * a.dtype.itemsize for a in ins)
    ins = [
        pltpu.with_memory_space_constraint(a, pltpu.HBM) if n in hbm else a
        for n, a in enumerate(ins)
    ]
    return pl.pallas_call(
        kernel,
        out_shape=outs,
        in_specs=[
            pl.BlockSpec(memory_space=pltpu.HBM) if n in hbm else vmem()
            for n in range(len(ins))
        ],
        out_specs=tuple(vmem() for _ in outs) if isinstance(outs, tuple) else vmem(),
        scratch_shapes=list(scratch),
        input_output_aliases=aliases or {},
        compiler_params=pltpu.CompilerParams(vmem_limit_bytes=limit * MIB),
        cost_estimate=pl.CostEstimate(
            flops=int(flops), bytes_accessed=bytes_accessed, transcendentals=0
        ),
    )(*ins)


def norm_act(values, gain):
    average = jnp.mean(values, axis=-1, keepdims=True)
    centred = values - average
    spread = jnp.mean(centred * centred, axis=-1, keepdims=True)
    half = centred * lax.rsqrt(spread + epsilon) * (0.5 * gain)
    return half + half * jnp.tanh(half)


def haar_cols(raw_ref, half):
    even = [raw_ref[:, q, pl.ds(0, half, stride=2), :] for q in range(raw_ref.shape[1])]
    odd = [raw_ref[:, q, pl.ds(1, half, stride=2), :] for q in range(raw_ref.shape[1])]
    return jnp.concatenate(even, -1), jnp.concatenate(odd, -1)


def prepare(values, gain, raw_ref, pad_ref, store, residual=None):
    _, width, channels = values.shape
    half = width // 2
    for q in range(channels // 128):
        raw_ref[:, q] = values[:, :, q * 128 : (q + 1) * 128].astype(jnp.float32)
    even, odd = haar_cols(raw_ref, half)
    if residual is not None:
        residual(0, even + odd)
        residual(1, even - odd)
    even, odd = norm_act(even, gain), norm_act(odd, gain)
    pad_ref[0, :, PAD : PAD + half, :] = odd
    pad_ref[1, :, PAD : PAD + half, :] = even
    store(0, pad_ref[0, :, PAD - 1 : PAD - 1 + half, :] - odd)
    store(1, even + odd)
    store(2, odd - even)
    store(3, even - pad_ref[1, :, PAD + 1 : PAD + 1 + half, :])


def clear_pads(pad_ref):
    rows, ext, channels = pad_ref.shape[1:]
    zero = jnp.zeros((rows, PAD, channels), jnp.float32)
    pad_ref[0, :, 0:PAD, :] = zero
    pad_ref[1, :, ext - PAD :, :] = zero


def norm_kernel(
    feat_hbm, gain_hbm, down_hbm, w_hbm, x_ref, res_ref, v_ref, g_ref, w_ref,
    feat_ref, gain_ref, down_ref, raw_ref, pad_ref, feat_sem, gain_sem, down_sem, w_sem,
    *, step
):
    frames, height, _, channels = feat_ref.shape
    feat_copies = [
        pltpu.make_async_copy(feat_hbm.at[f], feat_ref.at[f], feat_sem.at[f])
        for f in range(frames)
    ]
    w_copies = [pltpu.make_async_copy(w_hbm.at[a], w_ref.at[a], w_sem.at[a]) for a in range(3)]
    down_copy = pltpu.make_async_copy(down_hbm, down_ref, down_sem)
    gain_copy = pltpu.make_async_copy(gain_hbm, gain_ref, gain_sem)
    later_copies = [*w_copies, down_copy]
    for copy in (gain_copy, *feat_copies):
        copy.start()
    clear_pads(pad_ref)
    gain_copy.wait()
    gain = gain_ref[...]

    for f in range(frames):
        feat_copies[f].wait()
        if f == 0:
            for copy in later_copies:
                copy.start()

        def body(index, carry):
            h = index * step

            def store(t, value):
                x_ref[f, t, pl.ds(h + 1, step)] = value.astype(jnp.bfloat16)

            def residual(r, value):
                res_ref[f, r, pl.ds(h, step)] = value

            prepare(feat_ref[f, pl.ds(h, step)], gain, raw_ref, pad_ref, store, residual)
            return carry

        lax.fori_loop(0, height // step, body, 0)

    for a in range(3):
        w_copies[a].wait()

        def combine(b, carry):
            first, mid, last = (w_ref[a, b, c].astype(jnp.float32) for c in range(3))
            outer = first + last
            g_ref[a, b, 0] = (outer + mid).astype(jnp.bfloat16)
            g_ref[a, b, 1] = (outer - mid).astype(jnp.bfloat16)
            return carry

        lax.fori_loop(0, 3, combine, 0)

    down_copy.wait()
    rows = 32

    def fold(index, carry):
        r = pl.multiple_of(index * rows, rows)
        parts = [down_ref[s, pl.ds(r, rows), :].astype(jnp.float32) for s in range(8)]
        for bit in (4, 2):
            parts = [
                parts[s] + parts[s + bit] if not s & bit else parts[s - bit] - parts[s]
                for s in range(8)
            ]
        for s in range(8):
            v_ref[s, pl.ds(r, rows), :] = parts[s].astype(jnp.bfloat16)
        return carry

    lax.fori_loop(0, channels // rows, fold, 0)


def conv_pair(pair, x_ref, w_ref, g_ref, res_ref, v_ref, lev_ref, group):
    frames, _, ext, half, channels = x_ref.shape
    deep_rows = (ext - 2) // 2

    for index in range(deep_rows // group):
        start = 2 * group * index
        for i in range(2):
            f = 2 * pair + i
            taps = [a for a in range(3) if 0 <= f + a - 2 < frames]
            sums = []
            for t in range(4):
                total = None
                for a in taps:
                    for b in range(3):
                        rows = x_ref[f + a - 2, t, pl.ds(start + b, 2 * group)].reshape(
                            2 * group * half, channels
                        )
                        weight = (
                            w_ref[a, b, 0], g_ref[a, b, 0], g_ref[a, b, 1], w_ref[a, b, 2]
                        )[t]
                        part = jnp.dot(rows, weight, preferred_element_type=jnp.float32)
                        total = part if total is None else total + part
                sums.append(total)
            pieces = (sums[0] - sums[3] + sums[1], sums[0] + sums[3] + sums[2])
            for r in range(2):
                level = pieces[r].reshape(2 * group, half, channels)
                if res_ref is not None:
                    level = level + res_ref[f, r, pl.ds(start, 2 * group)]
                level = level.astype(jnp.bfloat16)
                for row in range(2 * group):
                    lev_ref[4 * i + 2 * (row % 2) + r, index * group + row // 2] = level[row]
    total = None
    for s in range(8):
        part = jnp.dot(
            lev_ref[s].reshape(deep_rows * half, channels),
            v_ref[s],
            preferred_element_type=jnp.float32,
        )
        total = part if total is None else total + part
    return total * haar_scale


def carry_kernel(
    x_in, near_ref, far_ref, gain_ref, w_ref, g_ref, v_ref, x_ref, out_ref,
    lev_ref, raw_ref, pad_ref, *, group
):
    frames, _, ext, _, _ = x_ref.shape
    gain = gain_ref[...]
    clear_pads(pad_ref)

    def halos(first, count):
        sides = by_side(near_ref[first : first + count, 0], far_ref[first : first + count, 0])
        for row, values in zip((0, ext - 1), sides):

            def store(t, value):
                for f in range(count):
                    x_ref[first + f, t, row] = value[f].astype(jnp.bfloat16)

            prepare(
                values, gain, raw_ref.at[first : first + count],
                pad_ref.at[:, first : first + count], store
            )

    halos(frames - 2, 2)
    projected = conv_pair(frames // 2, x_ref, w_ref, g_ref, None, v_ref, lev_ref, group)
    out_ref[...] = projected.reshape(out_ref.shape).astype(out_ref.dtype)
    halos(0, frames - 2)


def own_kernel(*refs, pair, extra, group, later):
    x_ref, res_ref, w_ref, g_ref, v_ref, wav_ref, inj_ref, gain_ref = refs[:8]
    carried_ref = refs[8] if extra else None
    later_refs = refs[8 + extra : 8 + extra + later]
    outs = refs[8 + extra + later :]
    deep_ref, lev_ref = outs[0], outs[-1]
    normed_refs = outs[1:-1]
    gain = gain_ref[...]
    injected = [
        lax.dot_general(
            wav_ref[pair, :, h, :],
            inj_ref[...],
            (((0,), (0,)), ((), ())),
            preferred_element_type=jnp.float32,
        )
        for h in range(wav_ref.shape[2])
    ]
    for ref, out in zip(later_refs, normed_refs[1:]):
        out[...] = norm_act(ref[...], gain).astype(out.dtype)
    value = conv_pair(pair, x_ref, w_ref, g_ref, res_ref, v_ref, lev_ref, group)
    value = value + jnp.concatenate(injected, 0)
    if extra:
        value = value + arrived(carried_ref[...].reshape(value.shape))
    deep_ref[...] = value.reshape(deep_ref.shape)
    if extra:
        normed_refs[0][...] = norm_act(value, gain).reshape(deep_ref.shape).astype(jnp.bfloat16)


def shifted(z_ref, sums):
    rows, ext = z_ref.shape[1:3]
    width = ext - 2 * PAD
    for c in range(3):
        z_ref[c, :, PAD : PAD + width, :] = sums[c].reshape(rows, width, -1)
    return (
        z_ref[0, :, PAD - 1 : PAD - 1 + width, :]
        + z_ref[1, :, PAD : PAD + width, :]
        + z_ref[2, :, PAD + 1 : PAD + 1 + width, :]
    )


def clear_columns(z_ref):
    rows, ext, channels = z_ref.shape[1:]
    zero = jnp.zeros((rows, PAD, channels), jnp.float32)
    z_ref[0, :, 0:PAD, :] = zero
    z_ref[2, :, ext - PAD :, :] = zero


def dot(rows, weight):
    return jnp.dot(rows, weight, preferred_element_type=jnp.float32)


def deep_conv(targets, ext_ref, w_ref, z_ref):
    frames, ext, width, channels = ext_ref.shape
    rows = ext - 2
    for target in targets:
        sums = []
        for c in range(3):
            total = None
            for a in range(3):
                source = target + a - 2
                if 0 <= source < frames:
                    for b in range(3):
                        part = dot(
                            ext_ref[source, b : b + rows].reshape(rows * width, channels),
                            w_ref[a, b, c],
                        )
                        total = part if total is None else total + part
            sums.append(total)
        yield target, shifted(z_ref, sums)


def deep_carry(rows, w_ref, z_ref, out_ref):
    both, last = [], []
    for c in range(3):
        first_tap, mid_tap = None, None
        for b in range(3):
            before, latest = rows(0, b), rows(1, b)
            part = dot(jnp.concatenate([before, latest], 0), w_ref[0, b, c])
            first_tap = part if first_tap is None else first_tap + part
            part = dot(latest, w_ref[1, b, c])
            mid_tap = part if mid_tap is None else mid_tap + part
        half = mid_tap.shape[0]
        both.append(first_tap[:half] + mid_tap)
        last.append(first_tap[half:])
    out_ref[0] = shifted(z_ref, both).astype(out_ref.dtype)
    out_ref[1] = shifted(z_ref, last).astype(out_ref.dtype)


def fill_ext(ext_ref, own_refs, near_ref, far_ref):
    frames, ext, _, _ = ext_ref.shape
    for f in range(frames):
        ext_ref[f, 1 : ext - 1] = own_refs[f][...]
        ext_ref[f, 0], ext_ref[f, ext - 1] = by_side(near_ref[f, 0], far_ref[f, 0])


def inner_carry_kernel(before_ref, latest_ref, w_ref, out_ref, z_ref):
    inner, _, channels = z_ref.shape[1:]
    clear_columns(z_ref)

    def rows(f, b):
        return (before_ref, latest_ref)[f][b : b + inner].reshape(-1, channels)

    deep_carry(rows, w_ref, z_ref, out_ref)


def outer_carry_kernel(
    before_ref, latest_ref, near_ref, far_ref, w_ref, out_ref, halo_ref, z_ref
):
    count = before_ref.shape[0]
    clear_columns(z_ref)
    first = near_ref.shape[0] - 2
    for f in range(2):
        halo_ref[f, 0], halo_ref[f, 1] = by_side(near_ref[first + f, 0], far_ref[first + f, 0])

    def one(f, r):
        if r < 0:
            return halo_ref[f, 0]
        if r >= count:
            return halo_ref[f, 1]
        return (before_ref, latest_ref)[f][r]

    def rows(f, b):
        return jnp.concatenate([one(f, b - 1), one(f, count + b - 2)], 0)

    deep_carry(rows, w_ref, z_ref, out_ref)


def deep_own_kernel(*refs, frames):
    own_refs = refs[:frames]
    feat_refs = refs[frames : 2 * frames]
    near_ref, far_ref, w_ref, out_ref, ext_ref, z_ref = refs[2 * frames :]
    clear_columns(z_ref)
    fill_ext(ext_ref, own_refs, near_ref, far_ref)
    for target, value in deep_conv(range(frames), ext_ref, w_ref, z_ref):
        out_ref[target] = value + feat_refs[target][...]


def arrived(values):
    values = values.astype(jnp.float32)
    return jnp.where(lax.axis_index("tm") == 0, jnp.zeros_like(values), values)


def join_kernel(own_ref, inner_ref, outer_ref, out_ref):
    frames, rows = own_ref.shape[:2]
    for f in range(frames):
        if f < 2:
            out_ref[f, 1 : rows - 1] = (
                own_ref[f, 1 : rows - 1] + arrived(inner_ref[f])
            ).astype(out_ref.dtype)
            for n, r in enumerate((0, rows - 1)):
                out_ref[f, r] = (own_ref[f, r] + arrived(outer_ref[f, n])).astype(out_ref.dtype)
        else:
            out_ref[f] = own_ref[f].astype(out_ref.dtype)


def chain(axis, wrap):
    count = lax.axis_size(axis)
    return [(i, (i + 1) % count) for i in range(count - 1 + wrap)]


def neighbours(axis):
    count = lax.axis_size(axis)
    routes = []
    for first in range(2):
        partner = {}
        for i in range(first, count - 1, 2):
            partner[i], partner[i + 1] = i + 1, i
        routes.append([(i, partner.get(i, i)) for i in range(count)])
    return routes


def by_side(near, far):
    index, count = lax.axis_index("rows"), lax.axis_size("rows")
    odd = lax.rem(index, 2) == 1
    above = jnp.where(odd, near, far)
    below = jnp.where(odd, far, near)
    above = jnp.where(index == 0, jnp.zeros_like(above), above)
    return above, jnp.where(index == count - 1, jnp.zeros_like(below), below)


def exchange(first_rows, last_rows):
    odd = lax.rem(lax.axis_index("rows"), 2) == 1
    routes = neighbours("rows")
    near = lax.ppermute(jnp.where(odd, first_rows, last_rows), "rows", routes[0])
    far = lax.ppermute(jnp.where(odd, last_rows, first_rows), "rows", routes[1])
    return near, far


def on_device(
    feat_mid, gain_mid, conv_mid, down_weight, wavelets, inject_weight, gain_deep, conv_deep
):
    frames, height, width, channels = feat_mid.shape
    deep_channels = down_weight.shape[-1]
    deep_frames, deep_rows, half = frames // 2, height // 2, width // 2
    group = 2 if deep_rows % 2 == 0 else 1
    bf16, f32 = jnp.bfloat16, jnp.float32
    shape = jax.ShapeDtypeStruct
    local = pltpu.VMEM
    gain_mid = gain_mid.reshape(1, -1)
    gain_deep = gain_deep.reshape(1, -1)

    near, far = exchange(feat_mid[:, :1], feat_mid[:, height - 1 :])
    x_shape = local((frames, 4, height + 2, half, channels), bf16)
    step = 4
    sem = pltpu.SemaphoreType.DMA
    x, residual, folded, mixed, conv_mid = call(
        functools.partial(norm_kernel, step=step),
        (
            x_shape,
            local((frames, 2, height, half, channels), f32),
            local(down_weight.shape, bf16),
            local((3, 3, 2) + conv_mid.shape[-2:], bf16),
            local(conv_mid.shape, bf16),
        ),
        (feat_mid, gain_mid, down_weight, conv_mid),
        (
            pltpu.VMEM(feat_mid.shape, bf16),
            pltpu.VMEM(gain_mid.shape, f32),
            pltpu.VMEM(down_weight.shape, bf16),
            pltpu.VMEM((step, channels // 128, width, 128), f32),
            pltpu.VMEM((2, step, half + 2 * PAD, channels), f32),
            sem((frames,)),
            sem(()),
            sem(()),
            sem((3,)),
        ),
        flops=5e9,
        hbm=(0, 1, 2, 3),
    )
    lev = pltpu.VMEM((8, deep_rows, half, channels), bf16)
    tap = 2 * height * width * channels * channels * 6
    proj = 2 * deep_rows * half * 8 * channels * deep_channels

    x, carry = call(
        functools.partial(carry_kernel, group=group),
        (x_shape, shape((deep_rows, half, deep_channels), bf16)),
        (x, near, far, gain_mid, conv_mid, mixed, folded),
        (
            lev,
            pltpu.VMEM((frames, channels // 128, width, 128), f32),
            pltpu.VMEM((2, frames, half + 2 * PAD, channels), f32),
        ),
        flops=3 * tap + proj,
        aliases={0: 0},
    )
    carried = lax.ppermute(carry, "tm", chain("tm", WRAPS[0]))
    deep = [None] * deep_frames
    for pair in reversed(range(deep_frames)):
        extra = pair == 0
        later = tuple(deep[1:]) if extra else ()
        made = call(
            functools.partial(own_kernel, pair=pair, extra=extra, group=group, later=len(later)),
            (shape((deep_rows, half, deep_channels), f32),)
            + (shape((deep_rows, half, deep_channels), bf16),) * (extra * deep_frames),
            (x, residual, conv_mid, mixed, folded, wavelets, inject_weight, gain_deep)
            + ((carried,) if extra else ())
            + later,
            (lev,),
            flops=(3 if extra else 6) * tap + proj,
        )
        deep[pair] = made[0]
    normed = made[1:]
    near, far = exchange(
        jnp.stack([n[:1] for n in normed]), jnp.stack([n[deep_rows - 1 :] for n in normed])
    )
    ext = pltpu.VMEM((deep_frames, deep_rows + 2, half, deep_channels), bf16)
    z = pltpu.VMEM((3, deep_rows, half + 2 * PAD, deep_channels), f32)
    tap = 2 * deep_rows * half * deep_channels * deep_channels * 9
    inner_z = pltpu.VMEM((3, deep_rows - 2, half + 2 * PAD, deep_channels), f32)
    outer_z = pltpu.VMEM((3, 2, half + 2 * PAD, deep_channels), f32)
    inner = call(
        inner_carry_kernel,
        shape((2, deep_rows - 2, half, deep_channels), bf16),
        (*normed[-2:], conv_deep),
        (inner_z,),
        flops=3 * tap * (deep_rows - 2) / deep_rows,
    )
    inner = lax.ppermute(inner, "tm", chain("tm", WRAPS[1]))
    outer = call(
        outer_carry_kernel,
        shape((2, 2, half, deep_channels), bf16),
        (*normed[-2:], near, far, conv_deep),
        (pltpu.VMEM((2, 2, half, deep_channels), bf16), outer_z),
        flops=3 * tap * 2 / deep_rows,
    )
    outer = lax.ppermute(outer, "tm", chain("tm", WRAPS[2]))
    own = call(
        functools.partial(deep_own_kernel, frames=deep_frames),
        shape((deep_frames, deep_rows, half, deep_channels), f32),
        (*normed, *deep, near, far, conv_deep),
        (ext, z),
        flops=(3 * deep_frames - 3) * tap,
    )
    return call(
        join_kernel,
        shape((deep_frames, deep_rows, half, deep_channels), bf16),
        (own, inner, outer),
    )


def solution(mesh):
    return jax.shard_map(
        on_device,
        mesh=mesh,
        in_specs=(
            P("tm", "rows", None, None),
            P(),
            P(),
            P(),
            P("tm", None, "rows", None),
            P(),
            P(),
            P(),
        ),
        out_specs=P("tm", "rows", None, None),
        check_vma=False,
    )
```

```python
import functools
import jax
import jax.numpy as jnp
from jax import lax
from jax.experimental import pallas as pl
from jax.experimental.pallas import tpu as pltpu
from jax.sharding import PartitionSpec as P

epsilon = 1e-06
haar_scale = 0.35355339059327373
PAD = 8
MIB = 1 << 20
WRAPS = (1, 1, 0)


def vmem():
    return pl.BlockSpec(memory_space=pltpu.VMEM)


def call(kernel, outs, ins, scratch=(), flops=0, limit=14, aliases=None, hbm=()):
    bytes_accessed = sum(int(a.size) * a.dtype.itemsize for a in ins)
    ins = [
        pltpu.with_memory_space_constraint(a, pltpu.HBM) if n in hbm else a
        for n, a in enumerate(ins)
    ]
    return pl.pallas_call(
        kernel,
        out_shape=outs,
        in_specs=[
            pl.BlockSpec(memory_space=pltpu.HBM) if n in hbm else vmem()
            for n in range(len(ins))
        ],
        out_specs=tuple(vmem() for _ in outs) if isinstance(outs, tuple) else vmem(),
        scratch_shapes=list(scratch),
        input_output_aliases=aliases or {},
        compiler_params=pltpu.CompilerParams(vmem_limit_bytes=limit * MIB),
        cost_estimate=pl.CostEstimate(
            flops=int(flops), bytes_accessed=bytes_accessed, transcendentals=0
        ),
    )(*ins)


def norm_act(values, gain):
    average = jnp.mean(values, axis=-1, keepdims=True)
    centred = values - average
    spread = jnp.mean(centred * centred, axis=-1, keepdims=True)
    half = centred * lax.rsqrt(spread + epsilon) * (0.5 * gain)
    return half + half * jnp.tanh(half)


def haar_cols(raw_ref, half):
    even = [raw_ref[:, q, pl.ds(0, half, stride=2), :] for q in range(raw_ref.shape[1])]
    odd = [raw_ref[:, q, pl.ds(1, half, stride=2), :] for q in range(raw_ref.shape[1])]
    return jnp.concatenate(even, -1), jnp.concatenate(odd, -1)


def prepare(values, gain, raw_ref, pad_ref, store, residual=None):
    _, width, channels = values.shape
    half = width // 2
    for q in range(channels // 128):
        raw_ref[:, q] = values[:, :, q * 128 : (q + 1) * 128].astype(jnp.float32)
    even, odd = haar_cols(raw_ref, half)
    if residual is not None:
        residual(0, even + odd)
        residual(1, even - odd)
    even, odd = norm_act(even, gain), norm_act(odd, gain)
    pad_ref[0, :, PAD : PAD + half, :] = odd
    pad_ref[1, :, PAD : PAD + half, :] = even
    store(0, pad_ref[0, :, PAD - 1 : PAD - 1 + half, :] - odd)
    store(1, even + odd)
    store(2, odd - even)
    store(3, even - pad_ref[1, :, PAD + 1 : PAD + 1 + half, :])


def clear_pads(pad_ref):
    rows, ext, channels = pad_ref.shape[1:]
    zero = jnp.zeros((rows, PAD, channels), jnp.float32)
    pad_ref[0, :, 0:PAD, :] = zero
    pad_ref[1, :, ext - PAD :, :] = zero


def rows_kernel(feat_hbm, gain_hbm, near_ref, far_ref, start_ref, gain_ref, sem):
    height = feat_hbm.shape[1]
    odd = lax.rem(lax.axis_index("rows"), 2)
    pairs = [
        (feat_hbm.at[:, pl.ds((height - 1) * use_last, 1)], ref)
        for ref, use_last in ((far_ref, odd), (near_ref, 1 - odd))
    ] + [(gain_hbm, gain_ref), (feat_hbm.at[0:1], start_ref)]
    copies = [pltpu.make_async_copy(src, dst, sem.at[n]) for n, (src, dst) in enumerate(pairs)]
    for copy in copies:
        copy.start()
    for copy in copies:
        copy.wait()


def norm_kernel(
    start_ref, gain_ref, feat_hbm, down_hbm, w_hbm, x_ref, res_ref, v_ref, g_ref, w_ref, lev_ref,
    own_lev_ref, feat_ref, down_ref, raw_ref, pad_ref, feat_sem, down_sem, w_sem, *, step
):
    _, height, _, channels = start_ref.shape
    frames = x_ref.shape[0]
    feat_copies = [
        pltpu.make_async_copy(feat_hbm.at[f], feat_ref.at[f - 1], feat_sem.at[f - 1])
        for f in range(1, frames)
    ]
    w_copies = [pltpu.make_async_copy(w_hbm.at[a], w_ref.at[a], w_sem.at[a]) for a in range(3)]
    down_copy = pltpu.make_async_copy(down_hbm, down_ref, down_sem)
    for copy in (*feat_copies, *w_copies, down_copy):
        copy.start()
    clear_pads(pad_ref)
    gain = gain_ref[...]

    for f in range(frames):
        frame_ref = start_ref.at[0] if f == 0 else feat_ref.at[f - 1]
        if f > 0:
            feat_copies[f - 1].wait()

        def body(index, carry):
            h = index * step

            def store(t, value):
                x_ref[f, t, pl.ds(h + 1, step)] = value.astype(jnp.bfloat16)

            def residual(r, value):
                res_ref[f, r, pl.ds(h, step)] = value

            prepare(frame_ref[pl.ds(h, step)], gain, raw_ref, pad_ref, store, residual)
            return carry

        lax.fori_loop(0, height // step, body, 0)

    for a in range(3):
        w_copies[a].wait()

        def combine(b, carry):
            first, mid, last = (w_ref[a, b, c].astype(jnp.float32) for c in range(3))
            outer = first + last
            g_ref[a, b, 0] = (outer + mid).astype(jnp.bfloat16)
            g_ref[a, b, 1] = (outer - mid).astype(jnp.bfloat16)
            return carry

        lax.fori_loop(0, 3, combine, 0)

    down_copy.wait()
    rows = 32

    def fold(index, carry):
        r = pl.multiple_of(index * rows, rows)
        parts = [down_ref[s, pl.ds(r, rows), :].astype(jnp.float32) for s in range(8)]
        for bit in (4, 2):
            parts = [
                parts[s] + parts[s + bit] if not s & bit else parts[s - bit] - parts[s]
                for s in range(8)
            ]
        for s in range(8):
            v_ref[s, pl.ds(r, rows), :] = parts[s].astype(jnp.bfloat16)
        return carry

    lax.fori_loop(0, channels // rows, fold, 0)
    inner, _ = groups_of(height // 2)
    for deep_rows in inner:
        conv_rows(frames // 2, deep_rows, x_ref, w_ref, g_ref, None, lev_ref)
        conv_rows(frames // 2 - 1, deep_rows, x_ref, w_ref, g_ref, res_ref, own_lev_ref, (0,))


def groups_of(deep_rows):
    inner = range(1, deep_rows - 1)
    return [tuple(inner[n : n + 2]) for n in range(0, len(inner), 2)], (0, deep_rows - 1)


def conv_rows(pair, deep_rows, x_ref, w_ref, g_ref, res_ref, lev_ref, parts=(0, 1)):
    frames, _, _, half, channels = x_ref.shape
    for i in parts:
        f = 2 * pair + i
        taps = [a for a in range(3) if 0 <= f + a - 2 < frames]
        sums = []
        for t in range(4):
            total = None
            for a in taps:
                for b in range(3):
                    rows = jnp.concatenate(
                        [
                            x_ref[f + a - 2, t, 2 * h + b : 2 * h + b + 2].reshape(
                                2 * half, channels
                            )
                            for h in deep_rows
                        ],
                        0,
                    )
                    weight = (w_ref[a, b, 0], g_ref[a, b, 0], g_ref[a, b, 1], w_ref[a, b, 2])[t]
                    part = dot(rows, weight)
                    total = part if total is None else total + part
            sums.append(total)
        pieces = (sums[0] - sums[3] + sums[1], sums[0] + sums[3] + sums[2])
        for r in range(2):
            for n, h in enumerate(deep_rows):
                for j in range(2):
                    at = (2 * n + j) * half
                    level = pieces[r][at : at + half]
                    if res_ref is not None:
                        level = level + res_ref[f, r, 2 * h + j]
                    lev_ref[4 * i + 2 * j + r, h] = level.astype(jnp.bfloat16)


def project(lev_ref, v_ref):
    total = None
    for s in range(8):
        part = dot(lev_ref[s].reshape(-1, lev_ref.shape[-1]), v_ref[s])
        total = part if total is None else total + part
    return total * haar_scale


def dot(rows, weight):
    return jnp.dot(rows, weight, preferred_element_type=jnp.float32)


def carry_kernel(
    x_in, lev_in, near_ref, far_ref, gain_ref, w_ref, g_ref, v_ref, x_ref, lev_ref, out_ref,
    raw_ref, pad_ref
):
    frames, _, ext, _, _ = x_ref.shape
    gain = gain_ref[...]
    clear_pads(pad_ref)

    def halos(first, count):
        sides = by_side(near_ref[first : first + count, 0], far_ref[first : first + count, 0])
        for row, values in zip((0, ext - 1), sides):

            def store(t, value):
                for f in range(count):
                    x_ref[first + f, t, row] = value[f].astype(jnp.bfloat16)

            prepare(
                values, gain, raw_ref.at[first : first + count],
                pad_ref.at[:, first : first + count], store
            )

    halos(frames - 2, 2)
    _, outer = groups_of((ext - 2) // 2)
    conv_rows(frames // 2, outer, x_ref, w_ref, g_ref, None, lev_ref)
    projected = project(lev_ref, v_ref)
    out_ref[...] = projected.reshape(out_ref.shape).astype(out_ref.dtype)
    halos(0, frames - 2)


def own_kernel(lev_in, x_ref, res_ref, w_ref, g_ref, v_ref, wav_ref, inj_ref, gain_ref, *outs):
    last_lev_ref, lev_ref = outs[0], outs[-1]
    deep_frames = wav_ref.shape[0]
    deep_refs, normed_refs = outs[1 : 1 + deep_frames], outs[1 + deep_frames : -1]
    gain = gain_ref[...]
    inner, outer = groups_of(lev_ref.shape[2])
    for pair in reversed(range(deep_frames)):
        last = pair == deep_frames - 1
        level = last_lev_ref if last else lev_ref.at[pair % 2]
        for deep_rows in inner:
            parts = (1,) if last else (0, 1)
            conv_rows(pair, deep_rows, x_ref, w_ref, g_ref, res_ref, level, parts)
        conv_rows(pair, outer, x_ref, w_ref, g_ref, res_ref, level)
        injected = [
            lax.dot_general(
                wav_ref[pair, :, h, :],
                inj_ref[...],
                (((0,), (0,)), ((), ())),
                preferred_element_type=jnp.float32,
            )
            for h in range(wav_ref.shape[2])
        ]
        value = project(level, v_ref) + jnp.concatenate(injected, 0)
        deep_refs[pair][...] = value.reshape(deep_refs[pair].shape)
        if pair > 0:
            out = normed_refs[pair - 1]
            out[...] = norm_act(value, gain).reshape(out.shape).astype(out.dtype)


def first_kernel(partial_ref, carried_ref, gain_ref, deep_ref, normed_ref):
    value = partial_ref[...] + arrived(carried_ref[...])
    deep_ref[...] = value
    normed_ref[...] = norm_act(value, gain_ref[...]).astype(normed_ref.dtype)


def shifted(z_ref, sums):
    rows, ext = z_ref.shape[1:3]
    width = ext - 2 * PAD
    for c in range(3):
        z_ref[c, :, PAD : PAD + width, :] = sums[c].reshape(rows, width, -1)
    return (
        z_ref[0, :, PAD - 1 : PAD - 1 + width, :]
        + z_ref[1, :, PAD : PAD + width, :]
        + z_ref[2, :, PAD + 1 : PAD + 1 + width, :]
    )


def clear_columns(z_ref):
    rows, ext, channels = z_ref.shape[1:]
    zero = jnp.zeros((rows, PAD, channels), jnp.float32)
    z_ref[0, :, 0:PAD, :] = zero
    z_ref[2, :, ext - PAD :, :] = zero


def deep_conv(targets, ext_ref, w_ref, z_ref):
    frames, ext, width, channels = ext_ref.shape
    rows = ext - 2
    for target in targets:
        sums = []
        for c in range(3):
            total = None
            for a in range(3):
                source = target + a - 2
                if 0 <= source < frames:
                    for b in range(3):
                        part = dot(
                            ext_ref[source, b : b + rows].reshape(rows * width, channels),
                            w_ref[a, b, c],
                        )
                        total = part if total is None else total + part
            sums.append(total)
        yield target, shifted(z_ref, sums)


def deep_carry(rows, w_ref, z_ref, out_ref):
    both, last = [], []
    for c in range(3):
        first_tap, mid_tap = None, None
        for b in range(3):
            before, latest = rows(0, b), rows(1, b)
            part = dot(jnp.concatenate([before, latest], 0), w_ref[0, b, c])
            first_tap = part if first_tap is None else first_tap + part
            part = dot(latest, w_ref[1, b, c])
            mid_tap = part if mid_tap is None else mid_tap + part
        half = mid_tap.shape[0]
        both.append(first_tap[:half] + mid_tap)
        last.append(first_tap[half:])
    out_ref[0] = shifted(z_ref, both).astype(out_ref.dtype)
    out_ref[1] = shifted(z_ref, last).astype(out_ref.dtype)


def fill_ext(ext_ref, own_refs, near_ref, far_ref):
    frames, ext, _, _ = ext_ref.shape
    for f in range(frames):
        ext_ref[f, 1 : ext - 1] = own_refs[f][...]
        ext_ref[f, 0], ext_ref[f, ext - 1] = by_side(near_ref[f, 0], far_ref[f, 0])


def inner_carry_kernel(before_ref, latest_ref, w_ref, out_ref, z_ref):
    inner, _, channels = z_ref.shape[1:]
    clear_columns(z_ref)

    def rows(f, b):
        return (before_ref, latest_ref)[f][b : b + inner].reshape(-1, channels)

    deep_carry(rows, w_ref, z_ref, out_ref)


def outer_carry_kernel(
    before_ref, latest_ref, near_ref, far_ref, w_ref, out_ref, halo_ref, z_ref
):
    count = before_ref.shape[0]
    clear_columns(z_ref)
    first = near_ref.shape[0] - 2
    for f in range(2):
        halo_ref[f, 0], halo_ref[f, 1] = by_side(near_ref[first + f, 0], far_ref[first + f, 0])

    def one(f, r):
        if r < 0:
            return halo_ref[f, 0]
        if r >= count:
            return halo_ref[f, 1]
        return (before_ref, latest_ref)[f][r]

    def rows(f, b):
        return jnp.concatenate([one(f, b - 1), one(f, count + b - 2)], 0)

    deep_carry(rows, w_ref, z_ref, out_ref)


def deep_own_kernel(*refs, frames):
    own_refs = refs[:frames]
    feat_refs = refs[frames : 2 * frames]
    near_ref, far_ref, w_ref, out_ref, ext_ref, z_ref = refs[2 * frames :]
    clear_columns(z_ref)
    fill_ext(ext_ref, own_refs, near_ref, far_ref)
    for target, value in deep_conv(range(frames), ext_ref, w_ref, z_ref):
        out_ref[target] = value + feat_refs[target][...]


def arrived(values):
    values = values.astype(jnp.float32)
    return jnp.where(lax.axis_index("tm") == 0, jnp.zeros_like(values), values)


def join_kernel(own_ref, inner_ref, outer_ref, out_ref):
    frames, rows = own_ref.shape[:2]
    for f in range(frames):
        if f < 2:
            out_ref[f, 1 : rows - 1] = (
                own_ref[f, 1 : rows - 1] + arrived(inner_ref[f])
            ).astype(out_ref.dtype)
            for n, r in enumerate((0, rows - 1)):
                out_ref[f, r] = (own_ref[f, r] + arrived(outer_ref[f, n])).astype(out_ref.dtype)
        else:
            out_ref[f] = own_ref[f].astype(out_ref.dtype)


def chain(axis, wrap):
    count = lax.axis_size(axis)
    return [(i, (i + 1) % count) for i in range(count - 1 + wrap)]


def neighbours(axis):
    count = lax.axis_size(axis)
    routes = []
    for first in range(2):
        partner = {}
        for i in range(first, count - 1, 2):
            partner[i], partner[i + 1] = i + 1, i
        routes.append([(i, partner.get(i, i)) for i in range(count)])
    return routes


def by_side(near, far):
    index, count = lax.axis_index("rows"), lax.axis_size("rows")
    odd = lax.rem(index, 2) == 1
    above = jnp.where(odd, near, far)
    below = jnp.where(odd, far, near)
    above = jnp.where(index == 0, jnp.zeros_like(above), above)
    return above, jnp.where(index == count - 1, jnp.zeros_like(below), below)


def exchange(near, far):
    routes = neighbours("rows")
    near = lax.ppermute(near, "rows", routes[0])
    far = lax.ppermute(far, "rows", routes[1])
    return near, far


def on_device(
    feat_mid, gain_mid, conv_mid, down_weight, wavelets, inject_weight, gain_deep, conv_deep
):
    frames, height, width, channels = feat_mid.shape
    deep_channels = down_weight.shape[-1]
    deep_frames, deep_rows, half = frames // 2, height // 2, width // 2
    bf16, f32 = jnp.bfloat16, jnp.float32
    shape = jax.ShapeDtypeStruct
    local = pltpu.VMEM
    gain_mid = gain_mid.reshape(1, -1)
    gain_deep = gain_deep.reshape(1, -1)

    rows_shape = shape((frames, 1, width, channels), bf16)
    near, far, start, gain_mid = call(
        rows_kernel,
        (
            rows_shape,
            rows_shape,
            local((1, height, width, channels), bf16),
            local(gain_mid.shape, f32),
        ),
        (feat_mid, gain_mid),
        (pltpu.SemaphoreType.DMA((4,)),),
        hbm=(0, 1),
    )
    near, far = exchange(near, far)
    x_shape = local((frames, 4, height + 2, half, channels), bf16)
    step = 4
    lev_shape = local((8, deep_rows, half, channels), bf16)
    sem = pltpu.SemaphoreType.DMA
    x, residual, folded, mixed, conv_mid, levels, own_levels = call(
        functools.partial(norm_kernel, step=step),
        (
            x_shape,
            local((frames, 2, height, half, channels), f32),
            local(down_weight.shape, bf16),
            local((3, 3, 2) + conv_mid.shape[-2:], bf16),
            local(conv_mid.shape, bf16),
            lev_shape,
            lev_shape,
        ),
        (start, gain_mid, feat_mid, down_weight, conv_mid),
        (
            pltpu.VMEM((frames - 1, height, width, channels), bf16),
            pltpu.VMEM(down_weight.shape, bf16),
            pltpu.VMEM((step, channels // 128, width, 128), f32),
            pltpu.VMEM((2, step, half + 2 * PAD, channels), f32),
            sem((frames - 1,)),
            sem(()),
            sem((3,)),
        ),
        flops=5e9,
        hbm=(2, 3, 4),
    )
    tap = 2 * height * width * channels * channels * 6
    proj = 2 * deep_rows * half * 8 * channels * deep_channels

    x, levels, carry = call(
        carry_kernel,
        (x_shape, lev_shape, shape((deep_rows, half, deep_channels), bf16)),
        (x, levels, near, far, gain_mid, conv_mid, mixed, folded),
        (
            pltpu.VMEM((frames, channels // 128, width, 128), f32),
            pltpu.VMEM((2, frames, half + 2 * PAD, channels), f32),
        ),
        flops=3 * tap + proj,
        aliases={0: 0, 1: 1},
    )
    carried = lax.ppermute(carry, "tm", chain("tm", WRAPS[0]))
    deep_shape = (deep_rows, half, deep_channels)
    _, *made = call(
        own_kernel,
        (lev_shape,)
        + (shape(deep_shape, f32),) * deep_frames
        + (shape(deep_shape, bf16),) * (deep_frames - 1),
        (own_levels, x, residual, conv_mid, mixed, folded, wavelets, inject_weight, gain_deep),
        (pltpu.VMEM((2, 8, deep_rows, half, channels), bf16),),
        flops=deep_frames * (6 * tap + proj) - 3 * tap,
        aliases={0: 0},
    )
    partial, *deep = made[:deep_frames]
    first, normed = call(
        first_kernel,
        (shape(deep_shape, f32), shape(deep_shape, bf16)),
        (partial, carried, gain_deep),
        flops=1e8,
    )
    deep, normed = [first, *deep], [normed, *made[deep_frames:]]
    odd = lax.rem(lax.axis_index("rows"), 2) == 1
    first = jnp.stack([n[:1] for n in normed])
    last = jnp.stack([n[deep_rows - 1 :] for n in normed])
    near, far = exchange(jnp.where(odd, first, last), jnp.where(odd, last, first))
    ext = pltpu.VMEM((deep_frames, deep_rows + 2, half, deep_channels), bf16)
    z = pltpu.VMEM((3, deep_rows, half + 2 * PAD, deep_channels), f32)
    tap = 2 * deep_rows * half * deep_channels * deep_channels * 9
    inner_z = pltpu.VMEM((3, deep_rows - 2, half + 2 * PAD, deep_channels), f32)
    outer_z = pltpu.VMEM((3, 2, half + 2 * PAD, deep_channels), f32)
    inner = call(
        inner_carry_kernel,
        shape((2, deep_rows - 2, half, deep_channels), bf16),
        (*normed[-2:], conv_deep),
        (inner_z,),
        flops=3 * tap * (deep_rows - 2) / deep_rows,
    )
    inner = lax.ppermute(inner, "tm", chain("tm", WRAPS[1]))
    outer = call(
        outer_carry_kernel,
        shape((2, 2, half, deep_channels), bf16),
        (*normed[-2:], near, far, conv_deep),
        (pltpu.VMEM((2, 2, half, deep_channels), bf16), outer_z),
        flops=3 * tap * 2 / deep_rows,
    )
    outer = lax.ppermute(outer, "tm", chain("tm", WRAPS[2]))
    own = call(
        functools.partial(deep_own_kernel, frames=deep_frames),
        shape((deep_frames, deep_rows, half, deep_channels), f32),
        (*normed, *deep, near, far, conv_deep),
        (ext, z),
        flops=(3 * deep_frames - 3) * tap,
    )
    return call(
        join_kernel,
        shape((deep_frames, deep_rows, half, deep_channels), bf16),
        (own, inner, outer),
    )


def solution(mesh):
    return jax.shard_map(
        on_device,
        mesh=mesh,
        in_specs=(
            P("tm", "rows", None, None),
            P(),
            P(),
            P(),
            P("tm", None, "rows", None),
            P(),
            P(),
            P(),
        ),
        out_specs=P("tm", "rows", None, None),
        check_vma=False,
    )
```

```python
import functools
import jax
import jax.numpy as jnp
from jax import lax
from jax.experimental import pallas as pl
from jax.experimental.pallas import tpu as pltpu
from jax.sharding import PartitionSpec as P

epsilon = 1e-06
haar_scale = 0.35355339059327373
PAD = 8
MIB = 1 << 20
WRAPS = (1, 1, 0)


def vmem():
    return pl.BlockSpec(memory_space=pltpu.VMEM)


def call(kernel, outs, ins, scratch=(), flops=0, limit=14, aliases=None, hbm=()):
    bytes_accessed = sum(int(a.size) * a.dtype.itemsize for a in ins)
    ins = [
        pltpu.with_memory_space_constraint(a, pltpu.HBM) if n in hbm else a
        for n, a in enumerate(ins)
    ]
    return pl.pallas_call(
        kernel,
        out_shape=outs,
        in_specs=[
            pl.BlockSpec(memory_space=pltpu.HBM) if n in hbm else vmem()
            for n in range(len(ins))
        ],
        out_specs=tuple(vmem() for _ in outs) if isinstance(outs, tuple) else vmem(),
        scratch_shapes=list(scratch),
        input_output_aliases=aliases or {},
        compiler_params=pltpu.CompilerParams(vmem_limit_bytes=limit * MIB),
        cost_estimate=pl.CostEstimate(
            flops=int(flops), bytes_accessed=bytes_accessed, transcendentals=0
        ),
    )(*ins)


def norm_act(values, gain):
    average = jnp.mean(values, axis=-1, keepdims=True)
    centred = values - average
    spread = jnp.mean(centred * centred, axis=-1, keepdims=True)
    half = centred * lax.rsqrt(spread + epsilon) * (0.5 * gain)
    return half + half * jnp.tanh(half)


def haar_cols(raw_ref, half):
    even = [raw_ref[:, q, pl.ds(0, half, stride=2), :] for q in range(raw_ref.shape[1])]
    odd = [raw_ref[:, q, pl.ds(1, half, stride=2), :] for q in range(raw_ref.shape[1])]
    return jnp.concatenate(even, -1), jnp.concatenate(odd, -1)


def prepare(values, gain, raw_ref, pad_ref, store, residual=None):
    _, width, channels = values.shape
    half = width // 2
    for q in range(channels // 128):
        raw_ref[:, q] = values[:, :, q * 128 : (q + 1) * 128].astype(jnp.float32)
    even, odd = haar_cols(raw_ref, half)
    if residual is not None:
        residual(0, even + odd)
        residual(1, even - odd)
    even, odd = norm_act(even, gain), norm_act(odd, gain)
    pad_ref[0, :, PAD : PAD + half, :] = odd
    pad_ref[1, :, PAD : PAD + half, :] = even
    store(0, pad_ref[0, :, PAD - 1 : PAD - 1 + half, :] - odd)
    store(1, even + odd)
    store(2, odd - even)
    store(3, even - pad_ref[1, :, PAD + 1 : PAD + 1 + half, :])


def clear_pads(pad_ref):
    rows, ext, channels = pad_ref.shape[1:]
    zero = jnp.zeros((rows, PAD, channels), jnp.float32)
    pad_ref[0, :, 0:PAD, :] = zero
    pad_ref[1, :, ext - PAD :, :] = zero


def rows_kernel(feat_hbm, gain_hbm, near_ref, far_ref, start_ref, gain_ref, sem):
    height = feat_hbm.shape[1]
    odd = lax.rem(lax.axis_index("rows"), 2)
    pairs = [
        (feat_hbm.at[:, pl.ds((height - 1) * use_last, 1)], ref)
        for ref, use_last in ((far_ref, odd), (near_ref, 1 - odd))
    ] + [(gain_hbm, gain_ref), (feat_hbm.at[pl.ds(feat_hbm.shape[0] - 2, 1)], start_ref)]
    copies = [pltpu.make_async_copy(src, dst, sem.at[n]) for n, (src, dst) in enumerate(pairs)]
    for copy in copies:
        copy.start()
    for copy in copies:
        copy.wait()


def norm_kernel(
    start_ref, gain_ref, feat_hbm, down_hbm, w_hbm, x_ref, res_ref, v_ref, g_ref, w_ref, lev_ref,
    own_lev_ref, feat_ref, down_ref, raw_ref, pad_ref, feat_sem, down_sem, w_sem, *, step
):
    _, height, _, channels = start_ref.shape
    frames = x_ref.shape[0]
    order = [frames - 2, frames - 1, *range(frames - 2)]
    feat_copies = [
        pltpu.make_async_copy(feat_hbm.at[f], feat_ref.at[n], feat_sem.at[n])
        for n, f in enumerate(order[1:])
    ]
    w_copies = [pltpu.make_async_copy(w_hbm.at[a], w_ref.at[a], w_sem.at[a]) for a in range(3)]
    down_copy = pltpu.make_async_copy(down_hbm, down_ref, down_sem)
    for copy in (*feat_copies, *w_copies, down_copy):
        copy.start()
    for n in range(2):
        clear_pads(pad_ref.at[n])
    gain = gain_ref[...]
    frame_refs = [start_ref.at[0], *(feat_ref.at[n] for n in range(frames - 1))]

    def rows_of(n, h, slot):
        f = order[n]

        def store(t, value):
            x_ref[f, t, pl.ds(h + 1, step)] = value.astype(jnp.bfloat16)

        def residual(r, value):
            res_ref[f, r, pl.ds(h, step)] = value

        values = frame_refs[n][pl.ds(h, step)]
        prepare(values, gain, raw_ref.at[slot], pad_ref.at[slot], store, residual)

    for n in range(2):
        if n > 0:
            feat_copies[n - 1].wait()

        def body(index, carry):
            rows_of(n, index * step, 0)
            return carry

        lax.fori_loop(0, height // step, body, 0)

    for a in range(3):
        w_copies[a].wait()

        def combine(b, carry):
            first, mid, last = (w_ref[a, b, c].astype(jnp.float32) for c in range(3))
            outer = first + last
            g_ref[a, b, 0] = (outer + mid).astype(jnp.bfloat16)
            g_ref[a, b, 1] = (outer - mid).astype(jnp.bfloat16)
            return carry

        lax.fori_loop(0, 3, combine, 0)

    for copy in (*feat_copies[1:], down_copy):
        copy.wait()
    rows, lanes = 16, 256

    def fold(r, q):
        parts = [down_ref[s, r : r + rows, q : q + lanes].astype(jnp.float32) for s in range(8)]
        for bit in (4, 2):
            parts = [
                parts[s] + parts[s + bit] if not s & bit else parts[s - bit] - parts[s]
                for s in range(8)
            ]
        for s in range(8):
            v_ref[s, r : r + rows, q : q + lanes] = parts[s].astype(jnp.bfloat16)

    inner, _ = groups_of(height // 2)
    norms = [
        functools.partial(rows_of, n, h, (h // step) % 2)
        for n in range(2, frames)
        for h in range(0, height, step)
    ]
    interleave(
        [
            one
            for deep_rows in inner
            for one in conv_steps(frames // 2, deep_rows, x_ref, w_ref, g_ref, None, lev_ref)
        ],
        norms,
    )
    interleave(
        [
            one
            for deep_rows in inner
            for one in conv_steps(
                frames // 2 - 1, deep_rows, x_ref, w_ref, g_ref, res_ref, own_lev_ref
            )
        ],
        [
            functools.partial(fold, r, q)
            for r in range(0, channels, rows)
            for q in range(0, down_ref.shape[-1], lanes)
        ],
    )


def groups_of(deep_rows):
    inner = range(1, deep_rows - 1)
    return [tuple(inner[n : n + 2]) for n in range(0, len(inner), 2)], (0, deep_rows - 1)


def conv_steps(pair, deep_rows, x_ref, w_ref, g_ref, res_ref, lev_ref):
    frames, _, _, half, channels = x_ref.shape

    def chain(sums, f, t):
        total = None
        for a in range(3):
            if not 0 <= f + a - 2 < frames:
                continue
            for b in range(3):
                rows = jnp.concatenate(
                    [
                        x_ref[f + a - 2, t, 2 * h + b : 2 * h + b + 2].reshape(2 * half, channels)
                        for h in deep_rows
                    ],
                    0,
                )
                weight = (w_ref[a, b, 0], g_ref[a, b, 0], g_ref[a, b, 1], w_ref[a, b, 2])[t]
                part = dot(rows, weight)
                total = part if total is None else total + part
        sums.append(total)

    def finish(sums, i):
        pieces = (sums[0] - sums[3] + sums[1], sums[0] + sums[3] + sums[2])
        for r in range(2):
            for n, h in enumerate(deep_rows):
                for j in range(2):
                    at = (2 * n + j) * half
                    level = pieces[r][at : at + half]
                    if res_ref is not None:
                        level = level + res_ref[2 * pair + i, r, 2 * h + j]
                    lev_ref[4 * i + 2 * j + r, h] = level.astype(jnp.bfloat16)

    steps = []
    for i in range(2):
        sums = []
        for t in range(4):
            steps.append(functools.partial(chain, sums, 2 * pair + i, t))
        steps.append(functools.partial(finish, sums, i))
    return steps


def conv_rows(*args):
    for step in conv_steps(*args):
        step()


def interleave(matrix_steps, vector_steps):
    done = 0
    for n, step in enumerate(matrix_steps):
        step()
        upto = len(vector_steps) * (n + 1) // len(matrix_steps)
        for other in vector_steps[done:upto]:
            other()
        done = upto


def project(lev_ref, v_ref):
    total = None
    for s in range(8):
        part = dot(lev_ref[s].reshape(-1, lev_ref.shape[-1]), v_ref[s])
        total = part if total is None else total + part
    return total * haar_scale


def dot(rows, weight):
    return jnp.dot(rows, weight, preferred_element_type=jnp.float32)


def carry_kernel(
    x_in, lev_in, near_ref, far_ref, gain_ref, w_ref, g_ref, v_ref, x_ref, lev_ref, out_ref,
    raw_ref, pad_ref
):
    frames, _, ext, _, _ = x_ref.shape
    gain = gain_ref[...]
    clear_pads(pad_ref)

    def halos(first, count):
        sides = by_side(near_ref[first : first + count, 0], far_ref[first : first + count, 0])
        for row, values in zip((0, ext - 1), sides):

            def store(t, value):
                for f in range(count):
                    x_ref[first + f, t, row] = value[f].astype(jnp.bfloat16)

            prepare(
                values, gain, raw_ref.at[first : first + count],
                pad_ref.at[:, first : first + count], store
            )

    halos(frames - 2, 2)
    _, outer = groups_of((ext - 2) // 2)
    conv_rows(frames // 2, outer, x_ref, w_ref, g_ref, None, lev_ref)
    projected = project(lev_ref, v_ref)
    out_ref[...] = projected.reshape(out_ref.shape).astype(out_ref.dtype)
    halos(0, frames - 2)


def own_kernel(lev_in, x_ref, res_ref, w_ref, g_ref, v_ref, wav_ref, inj_ref, gain_ref, *outs):
    last_lev_ref, lev_ref = outs[0], outs[-1]
    deep_frames = wav_ref.shape[0]
    deep_refs, normed_refs = outs[1 : 1 + deep_frames], outs[1 + deep_frames : -1]
    gain = gain_ref[...]
    inner, outer = groups_of(lev_ref.shape[2])
    for pair in reversed(range(deep_frames)):
        last = pair == deep_frames - 1
        level = last_lev_ref if last else lev_ref.at[pair % 2]
        for deep_rows in (outer,) if last else (*inner, outer):
            conv_rows(pair, deep_rows, x_ref, w_ref, g_ref, res_ref, level)
        injected = [
            lax.dot_general(
                wav_ref[pair, :, h, :],
                inj_ref[...],
                (((0,), (0,)), ((), ())),
                preferred_element_type=jnp.float32,
            )
            for h in range(wav_ref.shape[2])
        ]
        value = project(level, v_ref) + jnp.concatenate(injected, 0)
        deep_refs[pair][...] = value.reshape(deep_refs[pair].shape)
        if pair > 0:
            out = normed_refs[pair - 1]
            out[...] = norm_act(value, gain).reshape(out.shape).astype(out.dtype)


def first_kernel(partial_ref, carried_ref, gain_ref, deep_ref, normed_ref):
    value = partial_ref[...] + arrived(carried_ref[...])
    deep_ref[...] = value
    normed_ref[...] = norm_act(value, gain_ref[...]).astype(normed_ref.dtype)


def shifted(z_ref, sums):
    rows, ext = z_ref.shape[1:3]
    width = ext - 2 * PAD
    for c in range(3):
        z_ref[c, :, PAD : PAD + width, :] = sums[c].reshape(rows, width, -1)
    return (
        z_ref[0, :, PAD - 1 : PAD - 1 + width, :]
        + z_ref[1, :, PAD : PAD + width, :]
        + z_ref[2, :, PAD + 1 : PAD + 1 + width, :]
    )


def clear_columns(z_ref):
    rows, ext, channels = z_ref.shape[1:]
    zero = jnp.zeros((rows, PAD, channels), jnp.float32)
    z_ref[0, :, 0:PAD, :] = zero
    z_ref[2, :, ext - PAD :, :] = zero


def deep_conv(targets, ext_ref, w_ref, z_ref):
    frames, ext, width, channels = ext_ref.shape
    rows = ext - 2
    for target in targets:
        sums = []
        for c in range(3):
            total = None
            for a in range(3):
                source = target + a - 2
                if 0 <= source < frames:
                    for b in range(3):
                        part = dot(
                            ext_ref[source, b : b + rows].reshape(rows * width, channels),
                            w_ref[a, b, c],
                        )
                        total = part if total is None else total + part
            sums.append(total)
        yield target, shifted(z_ref, sums)


def deep_carry(rows, w_ref, z_ref, out_ref):
    both, last = [], []
    for c in range(3):
        first_tap, mid_tap = None, None
        for b in range(3):
            before, latest = rows(0, b), rows(1, b)
            part = dot(jnp.concatenate([before, latest], 0), w_ref[0, b, c])
            first_tap = part if first_tap is None else first_tap + part
            part = dot(latest, w_ref[1, b, c])
            mid_tap = part if mid_tap is None else mid_tap + part
        half = mid_tap.shape[0]
        both.append(first_tap[:half] + mid_tap)
        last.append(first_tap[half:])
    out_ref[0] = shifted(z_ref, both).astype(out_ref.dtype)
    out_ref[1] = shifted(z_ref, last).astype(out_ref.dtype)


def fill_ext(ext_ref, own_refs, near_ref, far_ref):
    frames, ext, _, _ = ext_ref.shape
    for f in range(frames):
        ext_ref[f, 1 : ext - 1] = own_refs[f][...]
        ext_ref[f, 0], ext_ref[f, ext - 1] = by_side(near_ref[f, 0], far_ref[f, 0])


def inner_carry_kernel(before_ref, latest_ref, w_ref, out_ref, z_ref):
    inner, _, channels = z_ref.shape[1:]
    clear_columns(z_ref)

    def rows(f, b):
        return (before_ref, latest_ref)[f][b : b + inner].reshape(-1, channels)

    deep_carry(rows, w_ref, z_ref, out_ref)


def outer_carry_kernel(
    before_ref, latest_ref, near_ref, far_ref, w_ref, out_ref, halo_ref, z_ref
):
    count = before_ref.shape[0]
    clear_columns(z_ref)
    first = near_ref.shape[0] - 2
    for f in range(2):
        halo_ref[f, 0], halo_ref[f, 1] = by_side(near_ref[first + f, 0], far_ref[first + f, 0])

    def one(f, r):
        if r < 0:
            return halo_ref[f, 0]
        if r >= count:
            return halo_ref[f, 1]
        return (before_ref, latest_ref)[f][r]

    def rows(f, b):
        return jnp.concatenate([one(f, b - 1), one(f, count + b - 2)], 0)

    deep_carry(rows, w_ref, z_ref, out_ref)


def deep_own_kernel(*refs, frames):
    own_refs = refs[:frames]
    feat_refs = refs[frames : 2 * frames]
    near_ref, far_ref, w_ref, out_ref, ext_ref, z_ref = refs[2 * frames :]
    clear_columns(z_ref)
    fill_ext(ext_ref, own_refs, near_ref, far_ref)
    for target, value in deep_conv(range(frames), ext_ref, w_ref, z_ref):
        out_ref[target] = value + feat_refs[target][...]


def arrived(values):
    values = values.astype(jnp.float32)
    return jnp.where(lax.axis_index("tm") == 0, jnp.zeros_like(values), values)


def join_kernel(own_ref, inner_ref, outer_ref, out_ref):
    frames, rows = own_ref.shape[:2]
    for f in range(frames):
        if f < 2:
            out_ref[f, 1 : rows - 1] = (
                own_ref[f, 1 : rows - 1] + arrived(inner_ref[f])
            ).astype(out_ref.dtype)
            for n, r in enumerate((0, rows - 1)):
                out_ref[f, r] = (own_ref[f, r] + arrived(outer_ref[f, n])).astype(out_ref.dtype)
        else:
            out_ref[f] = own_ref[f].astype(out_ref.dtype)


def chain(axis, wrap):
    count = lax.axis_size(axis)
    return [(i, (i + 1) % count) for i in range(count - 1 + wrap)]


def neighbours(axis):
    count = lax.axis_size(axis)
    routes = []
    for first in range(2):
        partner = {}
        for i in range(first, count - 1, 2):
            partner[i], partner[i + 1] = i + 1, i
        routes.append([(i, partner.get(i, i)) for i in range(count)])
    return routes


def by_side(near, far):
    index, count = lax.axis_index("rows"), lax.axis_size("rows")
    odd = lax.rem(index, 2) == 1
    above = jnp.where(odd, near, far)
    below = jnp.where(odd, far, near)
    above = jnp.where(index == 0, jnp.zeros_like(above), above)
    return above, jnp.where(index == count - 1, jnp.zeros_like(below), below)


def exchange(near, far):
    routes = neighbours("rows")
    near = lax.ppermute(near, "rows", routes[0])
    far = lax.ppermute(far, "rows", routes[1])
    return near, far


def on_device(
    feat_mid, gain_mid, conv_mid, down_weight, wavelets, inject_weight, gain_deep, conv_deep
):
    frames, height, width, channels = feat_mid.shape
    deep_channels = down_weight.shape[-1]
    deep_frames, deep_rows, half = frames // 2, height // 2, width // 2
    bf16, f32 = jnp.bfloat16, jnp.float32
    shape = jax.ShapeDtypeStruct
    local = pltpu.VMEM
    gain_mid = gain_mid.reshape(1, -1)
    gain_deep = gain_deep.reshape(1, -1)

    rows_shape = shape((frames, 1, width, channels), bf16)
    near, far, start, gain_mid = call(
        rows_kernel,
        (
            rows_shape,
            rows_shape,
            local((1, height, width, channels), bf16),
            local(gain_mid.shape, f32),
        ),
        (feat_mid, gain_mid),
        (pltpu.SemaphoreType.DMA((4,)),),
        hbm=(0, 1),
    )
    near, far = exchange(near, far)
    x_shape = local((frames, 4, height + 2, half, channels), bf16)
    step = 4
    lev_shape = local((8, deep_rows, half, channels), bf16)
    sem = pltpu.SemaphoreType.DMA
    x, residual, folded, mixed, conv_mid, levels, own_levels = call(
        functools.partial(norm_kernel, step=step),
        (
            x_shape,
            local((frames, 2, height, half, channels), f32),
            local(down_weight.shape, bf16),
            local((3, 3, 2) + conv_mid.shape[-2:], bf16),
            local(conv_mid.shape, bf16),
            lev_shape,
            lev_shape,
        ),
        (start, gain_mid, feat_mid, down_weight, conv_mid),
        (
            pltpu.VMEM((frames - 1, height, width, channels), bf16),
            pltpu.VMEM(down_weight.shape, bf16),
            pltpu.VMEM((2, step, channels // 128, width, 128), f32),
            pltpu.VMEM((2, 2, step, half + 2 * PAD, channels), f32),
            sem((frames - 1,)),
            sem(()),
            sem((3,)),
        ),
        flops=5e9,
        hbm=(2, 3, 4),
    )
    tap = 2 * height * width * channels * channels * 6
    proj = 2 * deep_rows * half * 8 * channels * deep_channels

    x, levels, carry = call(
        carry_kernel,
        (x_shape, lev_shape, shape((deep_rows, half, deep_channels), bf16)),
        (x, levels, near, far, gain_mid, conv_mid, mixed, folded),
        (
            pltpu.VMEM((frames, channels // 128, width, 128), f32),
            pltpu.VMEM((2, frames, half + 2 * PAD, channels), f32),
        ),
        flops=3 * tap + proj,
        aliases={0: 0, 1: 1},
    )
    carried = lax.ppermute(carry, "tm", chain("tm", WRAPS[0]))
    deep_shape = (deep_rows, half, deep_channels)
    _, *made = call(
        own_kernel,
        (lev_shape,)
        + (shape(deep_shape, f32),) * deep_frames
        + (shape(deep_shape, bf16),) * (deep_frames - 1),
        (own_levels, x, residual, conv_mid, mixed, folded, wavelets, inject_weight, gain_deep),
        (pltpu.VMEM((2, 8, deep_rows, half, channels), bf16),),
        flops=deep_frames * (6 * tap + proj) - 3 * tap,
        aliases={0: 0},
    )
    partial, *deep = made[:deep_frames]
    first, normed = call(
        first_kernel,
        (shape(deep_shape, f32), shape(deep_shape, bf16)),
        (partial, carried, gain_deep),
        flops=1e8,
    )
    deep, normed = [first, *deep], [normed, *made[deep_frames:]]
    odd = lax.rem(lax.axis_index("rows"), 2) == 1
    first = jnp.stack([n[:1] for n in normed])
    last = jnp.stack([n[deep_rows - 1 :] for n in normed])
    near, far = exchange(jnp.where(odd, first, last), jnp.where(odd, last, first))
    ext = pltpu.VMEM((deep_frames, deep_rows + 2, half, deep_channels), bf16)
    z = pltpu.VMEM((3, deep_rows, half + 2 * PAD, deep_channels), f32)
    tap = 2 * deep_rows * half * deep_channels * deep_channels * 9
    inner_z = pltpu.VMEM((3, deep_rows - 2, half + 2 * PAD, deep_channels), f32)
    outer_z = pltpu.VMEM((3, 2, half + 2 * PAD, deep_channels), f32)
    inner = call(
        inner_carry_kernel,
        shape((2, deep_rows - 2, half, deep_channels), bf16),
        (*normed[-2:], conv_deep),
        (inner_z,),
        flops=3 * tap * (deep_rows - 2) / deep_rows,
    )
    inner = lax.ppermute(inner, "tm", chain("tm", WRAPS[1]))
    outer = call(
        outer_carry_kernel,
        shape((2, 2, half, deep_channels), bf16),
        (*normed[-2:], near, far, conv_deep),
        (pltpu.VMEM((2, 2, half, deep_channels), bf16), outer_z),
        flops=3 * tap * 2 / deep_rows,
    )
    outer = lax.ppermute(outer, "tm", chain("tm", WRAPS[2]))
    own = call(
        functools.partial(deep_own_kernel, frames=deep_frames),
        shape((deep_frames, deep_rows, half, deep_channels), f32),
        (*normed, *deep, near, far, conv_deep),
        (ext, z),
        flops=(3 * deep_frames - 3) * tap,
    )
    return call(
        join_kernel,
        shape((deep_frames, deep_rows, half, deep_channels), bf16),
        (own, inner, outer),
    )


def solution(mesh):
    return jax.shard_map(
        on_device,
        mesh=mesh,
        in_specs=(
            P("tm", "rows", None, None),
            P(),
            P(),
            P(),
            P("tm", None, "rows", None),
            P(),
            P(),
            P(),
        ),
        out_specs=P("tm", "rows", None, None),
        check_vma=False,
    )
```

```python
import functools
import jax
import jax.numpy as jnp
from jax import lax
from jax.experimental import pallas as pl
from jax.experimental.pallas import tpu as pltpu
from jax.sharding import PartitionSpec as P

epsilon = 1e-06
haar_scale = 0.35355339059327373
PAD = 8
MIB = 1 << 20
WRAPS = (1, 1, 0)


def vmem():
    return pl.BlockSpec(memory_space=pltpu.VMEM)


def call(kernel, outs, ins, scratch=(), flops=0, limit=14, aliases=None, hbm=()):
    bytes_accessed = sum(int(a.size) * a.dtype.itemsize for a in ins)
    ins = [
        pltpu.with_memory_space_constraint(a, pltpu.HBM) if n in hbm else a
        for n, a in enumerate(ins)
    ]
    return pl.pallas_call(
        kernel,
        out_shape=outs,
        in_specs=[
            pl.BlockSpec(memory_space=pltpu.HBM) if n in hbm else vmem()
            for n in range(len(ins))
        ],
        out_specs=tuple(vmem() for _ in outs) if isinstance(outs, tuple) else vmem(),
        scratch_shapes=list(scratch),
        input_output_aliases=aliases or {},
        compiler_params=pltpu.CompilerParams(vmem_limit_bytes=limit * MIB),
        cost_estimate=pl.CostEstimate(
            flops=int(flops), bytes_accessed=bytes_accessed, transcendentals=0
        ),
    )(*ins)


def norm_act(values, gain):
    average = jnp.mean(values, axis=-1, keepdims=True)
    centred = values - average
    spread = jnp.mean(centred * centred, axis=-1, keepdims=True)
    half = centred * lax.rsqrt(spread + epsilon) * (0.5 * gain)
    return half + half * jnp.tanh(half)


def haar_cols(raw_ref, half):
    even = [raw_ref[:, q, pl.ds(0, half, stride=2), :] for q in range(raw_ref.shape[1])]
    odd = [raw_ref[:, q, pl.ds(1, half, stride=2), :] for q in range(raw_ref.shape[1])]
    return jnp.concatenate(even, -1), jnp.concatenate(odd, -1)


def prepare(values, gain, raw_ref, pad_ref, store, residual=None):
    _, width, channels = values.shape
    half = width // 2
    for q in range(channels // 128):
        raw_ref[:, q] = values[:, :, q * 128 : (q + 1) * 128].astype(jnp.float32)
    even, odd = haar_cols(raw_ref, half)
    if residual is not None:
        residual(0, even + odd)
        residual(1, even - odd)
    even, odd = norm_act(even, gain), norm_act(odd, gain)
    pad_ref[0, :, PAD : PAD + half, :] = odd
    pad_ref[1, :, PAD : PAD + half, :] = even
    store(0, pad_ref[0, :, PAD - 1 : PAD - 1 + half, :] - odd)
    store(1, even + odd)
    store(2, odd - even)
    store(3, even - pad_ref[1, :, PAD + 1 : PAD + 1 + half, :])


def clear_pads(pad_ref):
    rows, ext, channels = pad_ref.shape[1:]
    zero = jnp.zeros((rows, PAD, channels), jnp.float32)
    pad_ref[0, :, 0:PAD, :] = zero
    pad_ref[1, :, ext - PAD :, :] = zero


def rows_kernel(feat_hbm, gain_hbm, near_ref, far_ref, start_ref, gain_ref, sem):
    height = feat_hbm.shape[1]
    odd = lax.rem(lax.axis_index("rows"), 2)
    pairs = [
        (feat_hbm.at[:, pl.ds((height - 1) * use_last, 1)], ref)
        for ref, use_last in ((far_ref, odd), (near_ref, 1 - odd))
    ] + [(gain_hbm, gain_ref), (feat_hbm.at[pl.ds(feat_hbm.shape[0] - 2, 1)], start_ref)]
    copies = [pltpu.make_async_copy(src, dst, sem.at[n]) for n, (src, dst) in enumerate(pairs)]
    for copy in copies:
        copy.start()
    for copy in copies:
        copy.wait()


def norm_kernel(
    start_ref, gain_ref, feat_hbm, down_hbm, w_hbm, x_ref, res_ref, v_ref, g_ref, w_ref, lev_ref,
    own_lev_ref, feat_ref, down_ref, raw_ref, pad_ref, feat_sem, down_sem, w_sem, *, step
):
    _, height, _, channels = start_ref.shape
    frames = x_ref.shape[0]
    order = [frames - 2, frames - 1, *reversed(range(frames - 2))]
    feat_copies = [
        pltpu.make_async_copy(feat_hbm.at[f], feat_ref.at[n], feat_sem.at[n])
        for n, f in enumerate(order[1:])
    ]
    w_copies = [pltpu.make_async_copy(w_hbm.at[a], w_ref.at[a], w_sem.at[a]) for a in range(3)]
    down_copy = pltpu.make_async_copy(down_hbm, down_ref, down_sem)
    for copy in (feat_copies[0], *w_copies, *feat_copies[1:], down_copy):
        copy.start()
    for n in range(2):
        clear_pads(pad_ref.at[n])
    gain = gain_ref[...]
    frame_refs = [start_ref.at[0], *(feat_ref.at[n] for n in range(frames - 1))]

    def rows_of(n, h, slot):
        f = order[n]

        def store(t, value):
            x_ref[f, t, pl.ds(h + 1, step)] = value.astype(jnp.bfloat16)

        def residual(r, value):
            res_ref[f, r, pl.ds(h, step)] = value

        values = frame_refs[n][pl.ds(h, step)]
        prepare(values, gain, raw_ref.at[slot], pad_ref.at[slot], store, residual)

    for n in range(2):
        if n > 0:
            feat_copies[n - 1].wait()

        def body(index, carry):
            rows_of(n, index * step, 0)
            return carry

        lax.fori_loop(0, height // step, body, 0)

    for copy in w_copies:
        copy.wait()

    def combine(a, b, r):
        rows = slice(r, r + 32)
        first, mid, last = (w_ref[a, b, c, rows, :].astype(jnp.float32) for c in range(3))
        outer = first + last
        g_ref[a, b, 0, rows, :] = (outer + mid).astype(jnp.bfloat16)
        g_ref[a, b, 1, rows, :] = (outer - mid).astype(jnp.bfloat16)

    rows, lanes = 16, 256

    def fold(r, q):
        parts = [down_ref[s, r : r + rows, q : q + lanes].astype(jnp.float32) for s in range(8)]
        for bit in (4, 2):
            parts = [
                parts[s] + parts[s + bit] if not s & bit else parts[s - bit] - parts[s]
                for s in range(8)
            ]
        for s in range(8):
            v_ref[s, r : r + rows, q : q + lanes] = parts[s].astype(jnp.bfloat16)

    inner, _ = groups_of(height // 2)

    def norms(first, last):
        return [
            functools.partial(rows_of, n, h, (h // step) % 2)
            for n in range(first, last)
            for h in range(0, height, step)
        ]

    def steps(pair, level_ref, residual_ref, parts):
        both = [
            conv_steps(pair, deep_rows, x_ref, w_ref, g_ref, residual_ref, level_ref, parts)
            for deep_rows in inner
        ]
        return [sum(some, []) for some in zip(*both)]

    early, late = steps(frames // 2, lev_ref, None, (0, 1))
    interleave(
        early,
        [
            functools.partial(combine, a, b, r)
            for a in range(3)
            for b in range(3)
            for r in range(0, channels, 32)
        ],
    )
    for copy in (*feat_copies[1:], down_copy):
        copy.wait()
    interleave(late, norms(2, 3))
    interleave(sum(steps(frames // 2 - 1, own_lev_ref, res_ref, (1,)), []), norms(3, frames))
    interleave(
        sum(steps(frames // 2 - 1, own_lev_ref, res_ref, (0,)), []),
        [
            functools.partial(fold, r, q)
            for r in range(0, channels, rows)
            for q in range(0, down_ref.shape[-1], lanes)
        ],
    )


def groups_of(deep_rows):
    inner = range(1, deep_rows - 1)
    return [tuple(inner[n : n + 2]) for n in range(0, len(inner), 2)], (0, deep_rows - 1)


def conv_steps(pair, deep_rows, x_ref, w_ref, g_ref, res_ref, lev_ref, parts=(0, 1)):
    frames, _, _, half, channels = x_ref.shape

    def chain(sums, f, t):
        total = None
        for a in range(3):
            if not 0 <= f + a - 2 < frames:
                continue
            for b in range(3):
                rows = jnp.concatenate(
                    [
                        x_ref[f + a - 2, t, 2 * h + b : 2 * h + b + 2].reshape(2 * half, channels)
                        for h in deep_rows
                    ],
                    0,
                )
                weight = (w_ref[a, b, 0], g_ref[a, b, 0], g_ref[a, b, 1], w_ref[a, b, 2])[t]
                part = dot(rows, weight)
                total = part if total is None else total + part
        sums[t] = total

    def finish(sums, i):
        pieces = (sums[0] - sums[3] + sums[1], sums[0] + sums[3] + sums[2])
        for r in range(2):
            for n, h in enumerate(deep_rows):
                for j in range(2):
                    at = (2 * n + j) * half
                    level = pieces[r][at : at + half]
                    if res_ref is not None:
                        level = level + res_ref[2 * pair + i, r, 2 * h + j]
                    lev_ref[4 * i + 2 * j + r, h] = level.astype(jnp.bfloat16)

    early, late = [], []
    for i in parts:
        sums = {}
        early += [functools.partial(chain, sums, 2 * pair + i, t) for t in (0, 3)]
        late += [functools.partial(chain, sums, 2 * pair + i, t) for t in (1, 2)]
        late.append(functools.partial(finish, sums, i))
    return early, late


def conv_rows(*args):
    for i in range(2):
        early, late = conv_steps(*args, parts=(i,))
        for step in early + late:
            step()


def interleave(matrix_steps, vector_steps):
    done = 0
    for n, step in enumerate(matrix_steps):
        step()
        upto = len(vector_steps) * (n + 1) // len(matrix_steps)
        for other in vector_steps[done:upto]:
            other()
        done = upto


def project(lev_ref, v_ref):
    total = None
    for s in range(8):
        part = dot(lev_ref[s].reshape(-1, lev_ref.shape[-1]), v_ref[s])
        total = part if total is None else total + part
    return total * haar_scale


def dot(rows, weight):
    return jnp.dot(rows, weight, preferred_element_type=jnp.float32)


def carry_kernel(
    x_in, lev_in, near_ref, far_ref, gain_ref, w_ref, g_ref, v_ref, x_ref, lev_ref, out_ref,
    raw_ref, pad_ref
):
    frames, _, ext, _, _ = x_ref.shape
    gain = gain_ref[...]
    clear_pads(pad_ref)

    def halos(first, count):
        sides = by_side(near_ref[first : first + count, 0], far_ref[first : first + count, 0])
        for row, values in zip((0, ext - 1), sides):

            def store(t, value):
                for f in range(count):
                    x_ref[first + f, t, row] = value[f].astype(jnp.bfloat16)

            prepare(
                values, gain, raw_ref.at[first : first + count],
                pad_ref.at[:, first : first + count], store
            )

    halos(frames - 2, 2)
    _, outer = groups_of((ext - 2) // 2)
    conv_rows(frames // 2, outer, x_ref, w_ref, g_ref, None, lev_ref)
    projected = project(lev_ref, v_ref)
    out_ref[...] = projected.reshape(out_ref.shape).astype(out_ref.dtype)
    halos(0, frames - 2)


def own_kernel(lev_in, x_ref, res_ref, w_ref, g_ref, v_ref, wav_ref, inj_ref, gain_ref, *outs):
    last_lev_ref, lev_ref = outs[0], outs[-1]
    deep_frames = wav_ref.shape[0]
    deep_refs, normed_refs = outs[1 : 1 + deep_frames], outs[1 + deep_frames : -1]
    gain = gain_ref[...]
    inner, outer = groups_of(lev_ref.shape[2])
    for pair in reversed(range(deep_frames)):
        last = pair == deep_frames - 1
        level = last_lev_ref if last else lev_ref.at[pair % 2]
        for deep_rows in (outer,) if last else (*inner, outer):
            conv_rows(pair, deep_rows, x_ref, w_ref, g_ref, res_ref, level)
        injected = [
            lax.dot_general(
                wav_ref[pair, :, h, :],
                inj_ref[...],
                (((0,), (0,)), ((), ())),
                preferred_element_type=jnp.float32,
            )
            for h in range(wav_ref.shape[2])
        ]
        value = project(level, v_ref) + jnp.concatenate(injected, 0)
        deep_refs[pair][...] = value.reshape(deep_refs[pair].shape)
        if pair > 0:
            out = normed_refs[pair - 1]
            out[...] = norm_act(value, gain).reshape(out.shape).astype(out.dtype)


def first_kernel(partial_ref, carried_ref, gain_ref, deep_ref, normed_ref):
    value = partial_ref[...] + arrived(carried_ref[...])
    deep_ref[...] = value
    normed_ref[...] = norm_act(value, gain_ref[...]).astype(normed_ref.dtype)


def shifted(z_ref, sums):
    rows, ext = z_ref.shape[1:3]
    width = ext - 2 * PAD
    for c in range(3):
        z_ref[c, :, PAD : PAD + width, :] = sums[c].reshape(rows, width, -1)
    return (
        z_ref[0, :, PAD - 1 : PAD - 1 + width, :]
        + z_ref[1, :, PAD : PAD + width, :]
        + z_ref[2, :, PAD + 1 : PAD + 1 + width, :]
    )


def clear_columns(z_ref):
    rows, ext, channels = z_ref.shape[1:]
    zero = jnp.zeros((rows, PAD, channels), jnp.float32)
    z_ref[0, :, 0:PAD, :] = zero
    z_ref[2, :, ext - PAD :, :] = zero


def deep_conv(targets, ext_ref, w_ref, z_ref):
    frames, ext, width, channels = ext_ref.shape
    rows = ext - 2
    for target in targets:
        sums = []
        for c in range(3):
            total = None
            for a in range(3):
                source = target + a - 2
                if 0 <= source < frames:
                    for b in range(3):
                        part = dot(
                            ext_ref[source, b : b + rows].reshape(rows * width, channels),
                            w_ref[a, b, c],
                        )
                        total = part if total is None else total + part
            sums.append(total)
        yield target, shifted(z_ref, sums)


def deep_carry(rows, w_ref, z_ref, out_ref):
    both, last = [], []
    for c in range(3):
        first_tap, mid_tap = None, None
        for b in range(3):
            before, latest = rows(0, b), rows(1, b)
            part = dot(jnp.concatenate([before, latest], 0), w_ref[0, b, c])
            first_tap = part if first_tap is None else first_tap + part
            part = dot(latest, w_ref[1, b, c])
            mid_tap = part if mid_tap is None else mid_tap + part
        half = mid_tap.shape[0]
        both.append(first_tap[:half] + mid_tap)
        last.append(first_tap[half:])
    out_ref[0] = shifted(z_ref, both).astype(out_ref.dtype)
    out_ref[1] = shifted(z_ref, last).astype(out_ref.dtype)


def fill_ext(ext_ref, own_refs, near_ref, far_ref):
    frames, ext, _, _ = ext_ref.shape
    for f in range(frames):
        ext_ref[f, 1 : ext - 1] = own_refs[f][...]
        ext_ref[f, 0], ext_ref[f, ext - 1] = by_side(near_ref[f, 0], far_ref[f, 0])


def inner_carry_kernel(before_ref, latest_ref, w_ref, out_ref, z_ref):
    inner, _, channels = z_ref.shape[1:]
    clear_columns(z_ref)

    def rows(f, b):
        return (before_ref, latest_ref)[f][b : b + inner].reshape(-1, channels)

    deep_carry(rows, w_ref, z_ref, out_ref)


def outer_carry_kernel(
    before_ref, latest_ref, near_ref, far_ref, w_ref, out_ref, halo_ref, z_ref
):
    count = before_ref.shape[0]
    clear_columns(z_ref)
    first = near_ref.shape[0] - 2
    for f in range(2):
        halo_ref[f, 0], halo_ref[f, 1] = by_side(near_ref[first + f, 0], far_ref[first + f, 0])

    def one(f, r):
        if r < 0:
            return halo_ref[f, 0]
        if r >= count:
            return halo_ref[f, 1]
        return (before_ref, latest_ref)[f][r]

    def rows(f, b):
        return jnp.concatenate([one(f, b - 1), one(f, count + b - 2)], 0)

    deep_carry(rows, w_ref, z_ref, out_ref)


def deep_own_kernel(*refs, frames):
    own_refs = refs[:frames]
    feat_refs = refs[frames : 2 * frames]
    near_ref, far_ref, w_ref, out_ref, ext_ref, z_ref = refs[2 * frames :]
    clear_columns(z_ref)
    fill_ext(ext_ref, own_refs, near_ref, far_ref)
    for target, value in deep_conv(range(frames), ext_ref, w_ref, z_ref):
        out_ref[target] = value + feat_refs[target][...]


def arrived(values):
    values = values.astype(jnp.float32)
    return jnp.where(lax.axis_index("tm") == 0, jnp.zeros_like(values), values)


def join_kernel(own_ref, inner_ref, outer_ref, out_ref):
    frames, rows = own_ref.shape[:2]
    for f in range(frames):
        if f < 2:
            out_ref[f, 1 : rows - 1] = (
                own_ref[f, 1 : rows - 1] + arrived(inner_ref[f])
            ).astype(out_ref.dtype)
            for n, r in enumerate((0, rows - 1)):
                out_ref[f, r] = (own_ref[f, r] + arrived(outer_ref[f, n])).astype(out_ref.dtype)
        else:
            out_ref[f] = own_ref[f].astype(out_ref.dtype)


def chain(axis, wrap):
    count = lax.axis_size(axis)
    return [(i, (i + 1) % count) for i in range(count - 1 + wrap)]


def neighbours(axis):
    count = lax.axis_size(axis)
    routes = []
    for first in range(2):
        partner = {}
        for i in range(first, count - 1, 2):
            partner[i], partner[i + 1] = i + 1, i
        routes.append([(i, partner.get(i, i)) for i in range(count)])
    return routes


def by_side(near, far):
    index, count = lax.axis_index("rows"), lax.axis_size("rows")
    odd = lax.rem(index, 2) == 1
    above = jnp.where(odd, near, far)
    below = jnp.where(odd, far, near)
    above = jnp.where(index == 0, jnp.zeros_like(above), above)
    return above, jnp.where(index == count - 1, jnp.zeros_like(below), below)


def exchange(near, far):
    routes = neighbours("rows")
    near = lax.ppermute(near, "rows", routes[0])
    far = lax.ppermute(far, "rows", routes[1])
    return near, far


def on_device(
    feat_mid, gain_mid, conv_mid, down_weight, wavelets, inject_weight, gain_deep, conv_deep
):
    frames, height, width, channels = feat_mid.shape
    deep_channels = down_weight.shape[-1]
    deep_frames, deep_rows, half = frames // 2, height // 2, width // 2
    bf16, f32 = jnp.bfloat16, jnp.float32
    shape = jax.ShapeDtypeStruct
    local = pltpu.VMEM
    gain_mid = gain_mid.reshape(1, -1)
    gain_deep = gain_deep.reshape(1, -1)

    rows_shape = shape((frames, 1, width, channels), bf16)
    near, far, start, gain_mid = call(
        rows_kernel,
        (
            rows_shape,
            rows_shape,
            local((1, height, width, channels), bf16),
            local(gain_mid.shape, f32),
        ),
        (feat_mid, gain_mid),
        (pltpu.SemaphoreType.DMA((4,)),),
        hbm=(0, 1),
    )
    near, far = exchange(near, far)
    x_shape = local((frames, 4, height + 2, half, channels), bf16)
    step = 4
    lev_shape = local((8, deep_rows, half, channels), bf16)
    sem = pltpu.SemaphoreType.DMA
    x, residual, folded, mixed, conv_mid, levels, own_levels = call(
        functools.partial(norm_kernel, step=step),
        (
            x_shape,
            local((frames, 2, height, half, channels), f32),
            local(down_weight.shape, bf16),
            local((3, 3, 2) + conv_mid.shape[-2:], bf16),
            local(conv_mid.shape, bf16),
            lev_shape,
            lev_shape,
        ),
        (start, gain_mid, feat_mid, down_weight, conv_mid),
        (
            pltpu.VMEM((frames - 1, height, width, channels), bf16),
            pltpu.VMEM(down_weight.shape, bf16),
            pltpu.VMEM((2, step, channels // 128, width, 128), f32),
            pltpu.VMEM((2, 2, step, half + 2 * PAD, channels), f32),
            sem((frames - 1,)),
            sem(()),
            sem((3,)),
        ),
        flops=5e9,
        hbm=(2, 3, 4),
    )
    tap = 2 * height * width * channels * channels * 6
    proj = 2 * deep_rows * half * 8 * channels * deep_channels

    x, levels, carry = call(
        carry_kernel,
        (x_shape, lev_shape, shape((deep_rows, half, deep_channels), bf16)),
        (x, levels, near, far, gain_mid, conv_mid, mixed, folded),
        (
            pltpu.VMEM((frames, channels // 128, width, 128), f32),
            pltpu.VMEM((2, frames, half + 2 * PAD, channels), f32),
        ),
        flops=3 * tap + proj,
        aliases={0: 0, 1: 1},
    )
    carried = lax.ppermute(carry, "tm", chain("tm", WRAPS[0]))
    deep_shape = (deep_rows, half, deep_channels)
    _, *made = call(
        own_kernel,
        (lev_shape,)
        + (shape(deep_shape, f32),) * deep_frames
        + (shape(deep_shape, bf16),) * (deep_frames - 1),
        (own_levels, x, residual, conv_mid, mixed, folded, wavelets, inject_weight, gain_deep),
        (pltpu.VMEM((2, 8, deep_rows, half, channels), bf16),),
        flops=deep_frames * (6 * tap + proj) - 3 * tap,
        aliases={0: 0},
    )
    partial, *deep = made[:deep_frames]
    first, normed = call(
        first_kernel,
        (shape(deep_shape, f32), shape(deep_shape, bf16)),
        (partial, carried, gain_deep),
        flops=1e8,
    )
    deep, normed = [first, *deep], [normed, *made[deep_frames:]]
    odd = lax.rem(lax.axis_index("rows"), 2) == 1
    first = jnp.stack([n[:1] for n in normed])
    last = jnp.stack([n[deep_rows - 1 :] for n in normed])
    near, far = exchange(jnp.where(odd, first, last), jnp.where(odd, last, first))
    ext = pltpu.VMEM((deep_frames, deep_rows + 2, half, deep_channels), bf16)
    z = pltpu.VMEM((3, deep_rows, half + 2 * PAD, deep_channels), f32)
    tap = 2 * deep_rows * half * deep_channels * deep_channels * 9
    inner_z = pltpu.VMEM((3, deep_rows - 2, half + 2 * PAD, deep_channels), f32)
    outer_z = pltpu.VMEM((3, 2, half + 2 * PAD, deep_channels), f32)
    inner = call(
        inner_carry_kernel,
        shape((2, deep_rows - 2, half, deep_channels), bf16),
        (*normed[-2:], conv_deep),
        (inner_z,),
        flops=3 * tap * (deep_rows - 2) / deep_rows,
    )
    inner = lax.ppermute(inner, "tm", chain("tm", WRAPS[1]))
    outer = call(
        outer_carry_kernel,
        shape((2, 2, half, deep_channels), bf16),
        (*normed[-2:], near, far, conv_deep),
        (pltpu.VMEM((2, 2, half, deep_channels), bf16), outer_z),
        flops=3 * tap * 2 / deep_rows,
    )
    outer = lax.ppermute(outer, "tm", chain("tm", WRAPS[2]))
    own = call(
        functools.partial(deep_own_kernel, frames=deep_frames),
        shape((deep_frames, deep_rows, half, deep_channels), f32),
        (*normed, *deep, near, far, conv_deep),
        (ext, z),
        flops=(3 * deep_frames - 3) * tap,
    )
    return call(
        join_kernel,
        shape((deep_frames, deep_rows, half, deep_channels), bf16),
        (own, inner, outer),
    )


def solution(mesh):
    return jax.shard_map(
        on_device,
        mesh=mesh,
        in_specs=(
            P("tm", "rows", None, None),
            P(),
            P(),
            P(),
            P("tm", None, "rows", None),
            P(),
            P(),
            P(),
        ),
        out_specs=P("tm", "rows", None, None),
        check_vma=False,
    )
```
